256 devices in a mesh: rp: 64 (over y, x, z_hi, core), re: 4 (over z_lo).
Axes of the slice: x: 4, y: 4, z: 8 (z_hi: 2, z_lo: 4; z = z_hi * 4 + z_lo), core: 2. Of those that a mesh axis runs over, the one named last changes fastest.
Arguments:
- coupling: bfloat16 [1024, 4, 2, 6, 4096], P('rp', 're'), may hold values from -0.4375 to 0.4375
- rp_coords: int32 [3, 1024], P(None, 'rp'), may hold values from -8 to 8
- degeneracy: int32 [1024], P('rp'), may hold values from 1 to 8
- qpoints: int32 [3, 512], replicated, may hold values from 0 to 15
- eigvec: float32 [512, 2, 6, 6], P('rp'), may hold values from -1.75 to 1.75
Outputs:
- coupling_q: float32 [512, 4, 2, 6, 4096], P('rp', None, None, None, 're')
The draws below stay inside these ranges and needn't reach their ends.
All inputs are finite; a program needn't handle non-finite values.
Results may differ from the reference program's by a relative error of at most 0.0042.
Values may be sent and summed in bfloat16 or wider, within the bound.
A program may use at most 64 MiB of HBM per device.

```python
import math
import jax
import jax.numpy as jnp
from jax import lax

NW = 64
MODES = 6
QGRID = 16
RMAX = 8
RP = 1024
RE = 4
Q = 512


def plant(drawn, stream_key, smallest, top_value):
    longest = drawn.shape.index(max(drawn.shape))
    spots = []
    for shift in (0, 1):
        where = [jax.random.randint(jax.random.fold_in(stream_key, axis), (), 0, length) for axis, length in enumerate(drawn.shape)]
        where[longest] = (where[longest] + shift) % drawn.shape[longest]
        spots.append(tuple(where))
    return drawn.at[spots[0]].set(smallest).at[spots[1]].set(top_value)


def shard_levels(own_key, dims, pieces, low, top_value):
    gain = 1.0
    for dim, shards_of in pieces:
        steps = jax.random.uniform(jax.random.fold_in(jax.random.fold_in(own_key, 6), dim), (shards_of,), jnp.float32, low / len(pieces), top_value / len(pieces))
        gain = gain * jnp.repeat(jnp.exp(steps), dims[dim] // shards_of).reshape((-1,) + (1,) * (len(dims) - 1 - dim))
    return gain


def centred(rng, extent, width, bound, shards=(), dtype=jnp.bfloat16):
    result = width * jax.random.normal(rng, extent, jnp.float32)
    if shards:
        result = result * shard_levels(rng, extent, shards, -0.22, 0.18)
    return jnp.clip(result, -bound, bound).astype(dtype)


def setup_inputs(seed: int = 0) -> dict:
    streams_of = jax.random.split(jax.random.key(seed), 6)
    return {
        "coupling": centred(streams_of[0], (RP, RE, 2, MODES, NW * NW), (RP // 5) ** -0.5, 0.4375, ((0, 64), (1, 4))),
        "rp_coords": plant(jax.random.randint(streams_of[1], (3, RP), 0 - RMAX, RMAX + 1), jax.random.fold_in(streams_of[1], 1), 0 - RMAX, RMAX).astype(jnp.int32),
        "degeneracy": plant(jax.random.randint(streams_of[2], (RP,), 1, 9), jax.random.fold_in(streams_of[2], 1), 1, 8).astype(jnp.int32),
        "qpoints": plant(jax.random.randint(streams_of[3], (3, Q), 0, QGRID), jax.random.fold_in(streams_of[3], 1), 0, QGRID - 1).astype(jnp.int32),
        "eigvec": centred(streams_of[4], (Q, 2, MODES, MODES), (2 * MODES) ** -0.5, 1.75, ((0, 64),), jnp.float32),
    }


def phases(points, coords, degeneracy):
    turns = jnp.mod(points[0][:, None] * coords[0][None, :], QGRID)
    turns = turns + jnp.mod(points[1][:, None] * coords[1][None, :], QGRID)
    turns = turns + jnp.mod(points[2][:, None] * coords[2][None, :], QGRID)
    turns = jnp.mod(turns, QGRID)
    angles = turns.astype(jnp.float32) * (2.0 * math.pi / QGRID)
    weights = 1.0 / degeneracy.astype(jnp.float32)
    table = jnp.concatenate([jnp.cos(angles) * weights[None, :], jnp.sin(angles) * weights[None, :]], axis=0)
    return table.astype(jnp.bfloat16)


def combine(table, coupling):
    point_count = table.shape[0] // 2
    product = jnp.dot(table, coupling.reshape(coupling.shape[0], -1), preferred_element_type=jnp.float32)
    product = product.reshape((2, point_count) + coupling.shape[1:])
    real_part = product[0, :, :, 0] - product[1, :, :, 1]
    imag_part = product[0, :, :, 1] + product[1, :, :, 0]
    return jnp.stack([real_part, imag_part], axis=2)


def mode_mix(values, matrix):
    return jnp.einsum("qrkp,qkn->qrnp", values, matrix, precision=lax.Precision.HIGHEST)


def rotate(summed, eigvec):
    real_in = summed[:, :, 0]
    imag_in = summed[:, :, 1]
    vec_real = eigvec[:, 0]
    vec_imag = eigvec[:, 1]
    real_out = mode_mix(real_in, vec_real) - mode_mix(imag_in, vec_imag)
    imag_out = mode_mix(real_in, vec_imag) + mode_mix(imag_in, vec_real)
    return jnp.stack([real_out, imag_out], axis=2)


def reference(coupling, rp_coords, degeneracy, qpoints, eigvec):
    table = phases(qpoints, rp_coords, degeneracy)
    summed = combine(table, coupling)
    return rotate(summed, eigvec)
```

```python
import functools
import math

import numpy as np

import jax
import jax.numpy as jnp
from jax import lax
from jax.experimental import pallas as pl
from jax.experimental.pallas import tpu as pltpu
from jax.sharding import PartitionSpec as P

MESH = pl.DeviceIdType.MESH
UNITS = 6
PEERS = 32
STEP = ((0, 0, 1, 2, 2, 3), (0, 1, 1, 2, 3, 3))
WHICH = ((0, 2, 0, 0, 2, 0), (1, 1, 2, 1, 1, 2))
PLANE = ((0, 1), (1, 0), (0, 3), (3, 0), (1, 1), (3, 3), (1, 3), (3, 1), (0, 2), (2, 0), (1, 2), (2, 1), (3, 2), (2, 3), (2, 2))
SINE = np.linalg.solve(
    np.array([[w ** (2 * i + 1) for i in range(4)] for w in (1.0, 2.0, 3.0, 4.0)]),
    np.sin(np.pi / 8 * np.arange(1, 5)),
)


def place():
    rp, lo = lax.axis_index("rp"), lax.axis_index("re")
    return rp // 16, (rp // 4) % 4, (rp // 2) % 2, rp % 2, lo


def pick(table, core, unit):
    if isinstance(core, int):
        return table[core][unit]
    return jnp.where(core == 0, table[0][unit], table[1][unit])


def exchange(lat, qt, coupling, out, held, x, lattice, table, y, g, f,
             load_sem, own_sem, lat_sem, x_send, x_recv, y_send, y_recv, f_send, f_recv):
    row, col, hi, core, lo = place()
    chip = row * 4 + col
    me = chip * 2 + core

    def plane_peer(d):
        r, c = (row + d[0]) % 4, (col + d[1]) % 4
        return r * 4 + c

    def peers():
        yield chip, 1 - core
        for d in PLANE:
            for c in (0, 1):
                yield plane_peer(d), c

    def plane_id(i, c):
        return ((i * 2 + hi) * 2 + c, lo)

    def z_id(z_hi, z_lo):
        return ((chip * 2 + z_hi) * 2 + core, z_lo)

    load = pltpu.make_async_copy(coupling, held, load_sem)
    load.start()
    barrier = pltpu.get_barrier_semaphore()
    for i, c in peers():
        pl.semaphore_signal(barrier, inc=1, device_id=plane_id(i, c), device_id_type=MESH)
    for d in range(1, 8):
        z = (hi * 4 + lo + d) % 8
        pl.semaphore_signal(barrier, inc=1, device_id=z_id(z // 4, z % 4), device_id_type=MESH)
    lattice[me] = lat[...]
    pl.semaphore_wait(barrier, PEERS - 1 + 7)

    for i, c in peers():
        pltpu.make_async_remote_copy(
            lat, lattice.at[me], lat_sem.at[0], lat_sem.at[1],
            device_id=plane_id(i, c), device_id_type=MESH,
        ).start()
    load.wait()

    def piece(ref, i, c, unit):
        p = (lo + pick(STEP, c, unit)) % 4
        mode = (i // 8) * 3 + pick(WHICH, c, unit)
        return ref.at[:, mode, p * 8 + i % 8]

    for unit in range(UNITS):
        pltpu.make_async_copy(piece(coupling, chip, core, unit), x.at[unit, me], own_sem.at[unit]).start()
        for i, c in peers():
            pltpu.make_async_remote_copy(
                piece(held, i, c, unit), x.at[unit, me], x_send.at[unit], x_recv.at[unit],
                device_id=plane_id(i, c), device_id_type=MESH,
            ).start()

    def wait(ref, sem):
        pltpu.make_async_copy(ref, ref, sem).wait()

    wait(lattice.at[pl.ds(0, PEERS - 1)], lat_sem.at[1])
    groups = []
    for n in range(PEERS // 4):
        quad = lattice[4 * n : 4 * n + 4].astype(jnp.float32)
        groups.append(quad[0] + quad[1] + quad[2] + quad[3])
    vectors = jnp.concatenate(groups, axis=1)
    weights = 1.0 / vectors[5:6]
    vectors = vectors.astype(jnp.bfloat16)
    rows = 256
    for n in range(1024 // rows):
        turns = jnp.dot(qt[n * rows : (n + 1) * rows, :], vectors, preferred_element_type=jnp.float32)
        turns = turns - 16.0 * jnp.floor(turns * (1.0 / 16.0))
        w = jnp.abs(turns - 8.0) - 4.0
        s = w * w
        value = w * (((float(SINE[3]) * s + float(SINE[2])) * s + float(SINE[1])) * s + float(SINE[0]))
        table[n * rows : (n + 1) * rows, :] = (value * weights).astype(jnp.bfloat16)

    def transform(unit):
        wait(x.at[unit, 0], own_sem.at[unit])
        wait(x.at[unit, pl.ds(0, PEERS - 1)], x_recv.at[unit])
        part = jnp.dot(
            table[...], x.at[unit].reshape(1024, 128)[...], preferred_element_type=jnp.float32
        )
        y[unit] = part.astype(jnp.bfloat16).reshape(2, 512, 128)
        p = (lo + pick(STEP, core, unit)) % 4

        def send(z_hi):
            pltpu.make_async_remote_copy(
                y.at[unit, z_hi], g.at[unit, hi], y_send.at[unit, z_hi], y_recv.at[unit, hi],
                device_id=z_id(z_hi, p), device_id_type=MESH,
            ).start()

        def keep():
            g[unit, hi] = y[unit, hi]

        send(1 - hi)
        if unit == 0:
            keep()
        elif unit == 1:
            pl.when(core == 0)(keep)
            pl.when(core == 1)(lambda: send(hi))
        else:
            send(hi)

    def spread(unit):
        wait(g.at[unit, 1 - hi], y_recv.at[unit, 1 - hi])
        if unit == 1:
            pl.when(core == 1)(lambda: wait(g.at[unit, hi], y_recv.at[unit, hi]))
        elif unit > 1:
            wait(g.at[unit, hi], y_recv.at[unit, hi])
        total = g[unit, 0].astype(jnp.float32) + g[unit, 1].astype(jnp.float32)
        f.at[unit].reshape(512, 128)[...] = total.astype(jnp.bfloat16)
        re = (lo + 4 - pick(STEP, core, unit)) % 4
        mode = (chip // 8) * 3 + pick(WHICH, core, unit)
        place_of = out.at[:, re, mode, chip % 8]
        for i, c in peers():
            pltpu.make_async_remote_copy(
                f.at[unit, i * 2 + c], place_of, f_send.at[unit], f_recv.at[unit],
                device_id=plane_id(i, c), device_id_type=MESH,
            ).start()
        place_of[...] = f[unit, me]

    lag = 2
    for unit in range(UNITS):
        transform(unit)
        if unit >= lag:
            spread(unit - lag)
    for unit in range(UNITS - lag, UNITS):
        spread(unit)
    for unit in range(UNITS):
        wait(f.at[unit, pl.ds(0, PEERS - 1)], f_recv.at[unit])
    wait(lattice.at[pl.ds(0, PEERS - 1)], lat_sem.at[0])
    for unit in range(UNITS):
        wait(x.at[unit, pl.ds(0, PEERS - 1)], x_send.at[unit])
        wait(f.at[unit, pl.ds(0, PEERS - 1)], f_send.at[unit])
        wait(y.at[unit, 1 - hi], y_send.at[unit, 1 - hi])
        if unit == 1:
            pl.when(core == 1)(lambda: wait(y.at[unit, hi], y_send.at[unit, hi]))
        elif unit > 1:
            wait(y.at[unit, hi], y_send.at[unit, hi])


def rotate(vec, summed, out):
    q = pl.program_id(0)
    odd = lax.broadcasted_iota(jnp.int32, (16, 128), 0) % 2 == 1
    flat = summed.reshape(1, 4, 6, 16, 128)
    flat_out = out.reshape(1, 4, 6, 16, 128)
    for re in range(4):
        plain = [flat[0, re, k].astype(jnp.float32) for k in range(6)]
        turned = [jnp.where(odd, pltpu.roll(v, 1, 0), -pltpu.roll(v, 15, 0)) for v in plain]
        for n in range(6):
            total = None
            for k in range(6):
                term = vec[q, 0, k, n] * plain[k] + vec[q, 1, k, n] * turned[k]
                total = term if total is None else total + term
            flat_out[0, re, n] = total


def per_device(coupling, rp_coords, degeneracy, qpoints, eigvec):
    me = (lax.axis_index("rp") // 4) * 2 + lax.axis_index("rp") % 2
    lane = jnp.arange(128)
    ones = jnp.ones((1, 16), jnp.int32)
    stacked = jnp.concatenate([rp_coords, 0 * ones, ones, degeneracy[None], 0 * ones, 0 * ones], axis=0)
    lat = jnp.tile(jnp.repeat(stacked, 2, axis=1), (1, 4))
    lat = lat + jnp.where((jnp.arange(8) == 3)[:, None], 4 * (lane % 2)[None], 0)
    lat = jnp.where((lane // 32 == me % 4)[None], lat, 0).astype(jnp.bfloat16)
    points = qpoints.reshape(3, 16, 2, 2, 8).transpose(0, 2, 1, 3, 4).reshape(3, 512)
    points = jnp.repeat(points, 2, axis=1)
    unit_row = jnp.ones((1, 1024), jnp.int32)
    half = (-4 * (jnp.arange(1024) % 2))[None].astype(jnp.int32)
    qt = jnp.concatenate([points, unit_row, half, 0 * points], axis=0).T.astype(jnp.bfloat16)
    blocks = coupling.reshape(16, 2, 6, 32, 128).transpose(0, 2, 3, 1, 4)
    vmem = pl.BlockSpec(memory_space=pltpu.VMEM)
    dma = pltpu.SemaphoreType.DMA
    bf = jnp.bfloat16
    summed = pl.pallas_call(
        exchange,
        out_shape=jax.ShapeDtypeStruct((8, 4, 6, 8, 2, 128), bf),
        in_specs=[vmem, vmem, pl.BlockSpec(memory_space=pl.ANY)],
        out_specs=vmem,
        scratch_shapes=[
            pltpu.VMEM((16, 6, 32, 2, 128), bf),
            pltpu.VMEM((UNITS, PEERS, 16, 2, 128), bf),
            pltpu.VMEM((PEERS, 8, 128), bf),
            pltpu.VMEM((1024, 1024), bf),
            pltpu.VMEM((UNITS, 2, 512, 128), bf),
            pltpu.VMEM((UNITS, 2, 512, 128), bf),
            pltpu.VMEM((UNITS, PEERS, 8, 2, 128), bf),
            dma, dma((UNITS,)), dma((2,)), dma((UNITS,)), dma((UNITS,)),
            dma((UNITS, 2)), dma((UNITS, 2)), dma((UNITS,)), dma((UNITS,)),
        ],
        compiler_params=pltpu.CompilerParams(
            collective_id=0, has_side_effects=True, vmem_limit_bytes=40 * 2**20
        ),
        name="exchange",
    )(lat, qt, blocks)
    block = (1, 4, 6, 8, 2, 128)
    spec = pl.BlockSpec(block, lambda q: (q, 0, 0, 0, 0, 0))
    mixed = pl.pallas_call(
        rotate,
        grid=(8,),
        out_shape=jax.ShapeDtypeStruct((8, 4, 6, 8, 2, 128), jnp.float32),
        in_specs=[pl.BlockSpec(memory_space=pltpu.SMEM), spec],
        out_specs=spec,
        name="rotate",
    )(eigvec, summed)
    return mixed.transpose(0, 1, 4, 2, 3, 5).reshape(8, 4, 2, 6, 1024)


def solution(mesh):
    return jax.shard_map(
        per_device,
        mesh=mesh,
        in_specs=(
            P("rp", "re", None, None, None),
            P(None, "rp"),
            P("rp"),
            P(),
            P("rp", None, None, None),
        ),
        out_specs=P("rp", None, None, None, "re"),
        check_vma=False,
    )
```

```python
import functools
import math

import numpy as np

import jax
import jax.numpy as jnp
from jax import lax
from jax.experimental import pallas as pl
from jax.experimental.pallas import tpu as pltpu
from jax.sharding import PartitionSpec as P

MESH = pl.DeviceIdType.MESH
UNITS = 6
PEERS = 32
STEP = ((0, 0, 1, 3, 2, 2), (0, 3, 3, 1, 1, 2))
WHICH = ((0, 2, 0, 0, 0, 2), (1, 1, 2, 1, 2, 1))
PLANE = ((2, 2), (2, 1), (1, 2), (2, 3), (3, 2), (1, 1), (3, 3), (1, 3), (3, 1), (2, 0), (0, 2), (0, 1), (1, 0), (0, 3), (3, 0))
SINE = np.linalg.solve(
    np.array([[w ** (2 * i + 1) for i in range(4)] for w in (1.0, 2.0, 3.0, 4.0)]),
    np.sin(np.pi / 8 * np.arange(1, 5)),
)


def place():
    rp, lo = lax.axis_index("rp"), lax.axis_index("re")
    return rp // 16, (rp // 4) % 4, (rp // 2) % 2, rp % 2, lo


def pick(table, core, unit):
    if isinstance(core, int):
        return table[core][unit]
    return jnp.where(core == 0, table[0][unit], table[1][unit])


def exchange(coords_in, degeneracy_in, points_in, eigvec_in, coupling, out, coords, degeneracy, points, eigvec, held, x, own, lattice, table, y, g, f, summed, coef, doubled,
             load_sem, small_sem, lat_sem, x_send, x_recv, y_send, y_recv, f_send, f_recv):
    row, col, hi, core, lo = place()
    chip = row * 4 + col
    me = chip * 2 + core
    f32, bf16 = jnp.float32, jnp.bfloat16

    def plane_peer(d):
        r, c = (row + d[0]) % 4, (col + d[1]) % 4
        return r * 4 + c

    def peers():
        for c in (0, 1):
            for d in PLANE:
                yield plane_peer(d), c
        yield chip, 1 - core

    def plane_id(i, c):
        return ((i * 2 + hi) * 2 + c, lo)

    def z_id(z_hi, z_lo):
        return ((chip * 2 + z_hi) * 2 + core, z_lo)

    def iota(shape, dim):
        return lax.broadcasted_iota(jnp.int32, shape, dim)

    load = pltpu.make_async_copy(coupling, held, load_sem)
    small = [
        pltpu.make_async_copy(src, dst, small_sem.at[n])
        for n, (src, dst) in enumerate(
            ((coords_in, coords), (degeneracy_in, degeneracy), (points_in, points), (eigvec_in, eigvec))
        )
    ]
    for copy in small:
        copy.start()
    load.start()
    barrier = pltpu.get_barrier_semaphore()
    for i, c in peers():
        pl.semaphore_signal(barrier, inc=1, device_id=plane_id(i, c), device_id_type=MESH)
    for d in range(1, 8):
        z = (hi * 4 + lo + d) % 8
        pl.semaphore_signal(barrier, inc=1, device_id=z_id(z // 4, z % 4), device_id_type=MESH)

    for copy in small:
        copy.wait()
    zeros = functools.partial(jnp.zeros, dtype=f32)
    stacked = jnp.concatenate(
        [coords[...].astype(f32), zeros((2, 16)), degeneracy[...].astype(f32), zeros((2, 16))], axis=0
    )
    spread16 = (iota((16, 128), 0) == iota((16, 128), 1) % 32 // 2).astype(f32)
    lat = jnp.dot(stacked, spread16, preferred_element_type=f32)
    line, lane = iota((8, 128), 0), iota((8, 128), 1)
    lat = lat + jnp.where(line == 3, 4 * (lane % 2), jnp.where(line == 4, 1, 0)).astype(f32)
    own[...] = jnp.where(lane // 32 == me % 4, lat, 0.0).astype(bf16)
    lattice[me] = own[...]
    grid = jnp.concatenate([points[...].astype(f32), zeros((5, 512))], axis=0)
    twice = []
    lane = iota((128, 256), 1)
    pair = (iota((128, 256), 0) == lane % 128 // 32 * 32 + lane // 128 * 16 + lane % 32 // 2).astype(f32)
    for n in range(4):
        twice.append(jnp.dot(grid[:, 128 * n : 128 * n + 128], pair, preferred_element_type=f32))
    line, lane = iota((8, 512), 0), iota((8, 512), 1)
    extra = jnp.where(line == 3, 1, jnp.where(line == 4, -4 * (lane % 2), 0)).astype(f32)
    for h in range(2):
        doubled[h] = jnp.concatenate([t[:, 128 * h : 128 * h + 128] for t in twice], axis=1) + extra
    rows16 = (iota((16, 8), 0) // 2 == iota((16, 8), 1)).astype(f32)
    columns = lax.dot_general(
        rows16, eigvec[...], (((1,), (1,)), ((), ())), precision=lax.Precision.HIGHEST, preferred_element_type=f32
    )
    for n in range(72):
        coef[n] = jnp.broadcast_to(columns[:, n : n + 1], (16, 128))

    pl.semaphore_wait(barrier, PEERS - 1 + 7)

    for i, c in peers():
        pltpu.make_async_remote_copy(
            own, lattice.at[me], lat_sem.at[0], lat_sem.at[1],
            device_id=plane_id(i, c), device_id_type=MESH,
        ).start()
    load.wait()

    def piece(ref, i, c, unit):
        p = (lo + pick(STEP, c, unit)) % 4
        mode = (i // 8) * 3 + pick(WHICH, c, unit)
        return ref.at[:, mode, p * 8 + i % 8]

    for unit in range(UNITS):
        for i, c in peers():
            pltpu.make_async_remote_copy(
                piece(held, i, c, unit), x.at[unit, me], x_send.at[unit], x_recv.at[unit],
                device_id=plane_id(i, c), device_id_type=MESH,
            ).start()
    for unit in range(UNITS):
        x[unit, me] = piece(held, chip, core, unit)[...]

    def wait(ref, sem):
        pltpu.make_async_copy(ref, ref, sem).wait()

    wait(lattice.at[pl.ds(0, PEERS - 1)], lat_sem.at[1])
    groups = []
    for n in range(PEERS // 4):
        quad = lattice[4 * n : 4 * n + 4].astype(f32)
        groups.append(quad[0] + quad[1] + quad[2] + quad[3])
    vectors = jnp.concatenate(groups, axis=1)
    weights = 1.0 / vectors[5:6]
    def tabulate(half):
        for n in range(2):
            turns = lax.dot_general(
                doubled.at[half][:, n * 256 : (n + 1) * 256], vectors,
                (((0,), (0,)), ((), ())), preferred_element_type=f32,
            )
            turns = turns - 16.0 * jnp.floor(turns * (1.0 / 16.0))
            w = jnp.abs(turns - 8.0) - 4.0
            s = w * w
            value = w * (((float(SINE[3]) * s + float(SINE[2])) * s + float(SINE[1])) * s + float(SINE[0]))
            table.at[half][n * 256 : (n + 1) * 256, :] = (value * weights).astype(bf16)

    def send(unit, half):
        p = (lo + pick(STEP, core, unit)) % 4
        pltpu.make_async_remote_copy(
            y.at[unit, half], g.at[unit, hi], y_send.at[unit, half], y_recv.at[unit, hi],
            device_id=z_id(half, p), device_id_type=MESH,
        ).start()

    def contract(unit, half, target):
        part = jnp.dot(table[half], x.at[unit].reshape(1024, 128)[...], preferred_element_type=f32)
        target[...] = part.astype(bf16)

    def transform(unit):
        wait(x.at[unit, pl.ds(0, PEERS - 1)], x_recv.at[unit])
        contract(unit, 1 - hi, y.at[unit, 1 - hi])
        send(unit, 1 - hi)
        if unit == 0:
            tabulate(hi)
            contract(unit, hi, g.at[unit, hi])
        elif unit == 1:
            contract(unit, hi, y.at[unit, hi])

            @pl.when(core == 0)
            def keep():
                g[unit, hi] = y[unit, hi]

            pl.when(core == 1)(lambda: send(unit, hi))
        else:
            contract(unit, hi, y.at[unit, hi])
            send(unit, hi)

    tabulate(1 - hi)

    def spread(unit):
        wait(g.at[unit, 1 - hi], y_recv.at[unit, 1 - hi])
        if unit == 1:
            pl.when(core == 1)(lambda: wait(g.at[unit, hi], y_recv.at[unit, hi]))
        elif unit > 1:
            wait(g.at[unit, hi], y_recv.at[unit, hi])
        total = g[unit, 0].astype(f32) + g[unit, 1].astype(f32)
        f[unit * PEERS : (unit + 1) * PEERS] = total.astype(bf16).reshape(PEERS, 16, 128)
        step = pick(STEP, core, unit)
        mode = (chip // 8) * 3 + pick(WHICH, core, unit)
        place_of = summed.at[step, mode, chip % 8]
        for i, c in peers():
            pltpu.make_async_remote_copy(
                f.at[unit * PEERS + i * 2 + c], place_of, f_send.at[unit], f_recv.at[step],
                device_id=plane_id(i, c), device_id_type=MESH,
            ).start()
        place_of[...] = f[unit * PEERS + me]

    odd = iota((16, 128), 0) % 2 == 1

    def rotate(step):
        for c in (0, 1):
            mine = 2 if c == step % 2 else 1
            pl.when(core == c)(lambda: wait(f.at[pl.ds(0, 48 - mine)], f_recv.at[step]))
        re = (lo + 4 - step) % 4

        def block(b, _):
            plain = [summed[step, k, b].astype(f32) for k in range(6)]
            turned = [jnp.where(odd, pltpu.roll(v, 1, 0), -pltpu.roll(v, 15, 0)) for v in plain]
            for n in range(6):
                total = None
                for k in range(6):
                    at = (k * 6 + n) * 2
                    term = coef[at] * plain[k] + coef[at + 1] * turned[k]
                    total = term if total is None else total + term
                out[:, re, n, b] = total.reshape(8, 2, 128)
            return 0

        lax.fori_loop(0, 8, block, 0)

    lag = 4
    for unit in range(UNITS):
        transform(unit)
        if unit >= lag:
            spread(unit - lag)
    for unit in range(UNITS - lag, UNITS):
        spread(unit)
    wait(lattice.at[pl.ds(0, PEERS - 1)], lat_sem.at[0])
    for unit in range(UNITS):
        wait(x.at[unit, pl.ds(0, PEERS - 1)], x_send.at[unit])
        wait(g.at[unit, 0], y_send.at[unit, 1 - hi])
        if unit == 1:
            pl.when(core == 1)(lambda: wait(g.at[unit, 0], y_send.at[unit, hi]))
        elif unit > 1:
            wait(g.at[unit, 0], y_send.at[unit, hi])
    for step in (0, 3, 1, 2):
        rotate(step)
    for unit in range(UNITS):
        wait(f.at[pl.ds(0, PEERS - 1)], f_send.at[unit])


def per_device(coupling, rp_coords, degeneracy, qpoints, eigvec):
    blocks = coupling.reshape(16, 2, 6, 32, 128).transpose(0, 2, 3, 1, 4)
    vectors = eigvec.transpose(2, 3, 1, 0).reshape(72, 8)
    vmem = pl.BlockSpec(memory_space=pltpu.VMEM)
    dma = pltpu.SemaphoreType.DMA
    bf = jnp.bfloat16
    mixed = pl.pallas_call(
        exchange,
        out_shape=jax.ShapeDtypeStruct((8, 4, 6, 8, 2, 128), jnp.float32),
        in_specs=[pl.BlockSpec(memory_space=pl.ANY)] * 5,
        out_specs=vmem,
        scratch_shapes=[
            pltpu.VMEM((3, 16), jnp.int32),
            pltpu.VMEM((1, 16), jnp.int32),
            pltpu.VMEM((3, 512), jnp.int32),
            pltpu.VMEM((72, 8), jnp.float32),
            pltpu.VMEM((16, 6, 32, 2, 128), bf),
            pltpu.VMEM((UNITS, PEERS, 16, 2, 128), bf),
            pltpu.VMEM((8, 128), bf),
            pltpu.VMEM((PEERS, 8, 128), bf),
            pltpu.VMEM((2, 512, 1024), bf),
            pltpu.VMEM((UNITS, 2, 512, 128), bf),
            pltpu.VMEM((UNITS, 2, 512, 128), bf),
            pltpu.VMEM((UNITS * PEERS, 16, 128), bf),
            pltpu.VMEM((4, 6, 8, 16, 128), bf),
            pltpu.VMEM((72, 16, 128), jnp.float32),
            pltpu.VMEM((2, 8, 512), jnp.float32),
            dma, dma((4,)), dma((2,)), dma((UNITS,)), dma((UNITS,)),
            dma((UNITS, 2)), dma((UNITS, 2)), dma((UNITS,)), dma((4,)),
        ],
        compiler_params=pltpu.CompilerParams(
            collective_id=0, has_side_effects=True, vmem_limit_bytes=40 * 2**20
        ),
        name="exchange",
    )(*(pltpu.with_memory_space_constraint(v, pltpu.HBM) for v in (rp_coords, degeneracy.reshape(1, 16), qpoints, vectors, blocks)))
    return mixed.transpose(0, 1, 4, 2, 3, 5).reshape(8, 4, 2, 6, 1024)


def solution(mesh):
    return jax.shard_map(
        per_device,
        mesh=mesh,
        in_specs=(
            P("rp", "re", None, None, None),
            P(None, "rp"),
            P("rp"),
            P(),
            P("rp", None, None, None),
        ),
        out_specs=P("rp", None, None, None, "re"),
        check_vma=False,
    )
```

```python
import functools
import math

import numpy as np

import jax
import jax.numpy as jnp
from jax import lax
from jax.experimental import pallas as pl
from jax.experimental.pallas import tpu as pltpu
from jax.sharding import PartitionSpec as P

MESH = pl.DeviceIdType.MESH
UNITS = 6
PEERS = 32
LATE = (3, 4, 5)
JOINT = 5
EARLY = 3
STEP = ((0, 0, 2, 3, 1, 2), (0, 3, 1, 3, 1, 2))
WHICH = ((0, 2, 0, 0, 0, 2), (1, 2, 2, 1, 1, 1))
PLANE = ((2, 2), (2, 1), (1, 2), (2, 3), (3, 2), (1, 1), (3, 3), (1, 3), (3, 1), (2, 0), (0, 2), (0, 1), (1, 0), (0, 3), (3, 0))
SINE = np.linalg.solve(
    np.array([[w ** (2 * i + 1) for i in range(4)] for w in (1.0, 2.0, 3.0, 4.0)]),
    np.sin(np.pi / 8 * np.arange(1, 5)),
)


def place():
    rp, lo = lax.axis_index("rp"), lax.axis_index("re")
    return rp // 16, (rp // 4) % 4, (rp // 2) % 2, rp % 2, lo


def pick(table, core, unit):
    if isinstance(core, int):
        return table[core][unit]
    return jnp.where(core == 0, table[0][unit], table[1][unit])


def exchange(coords_in, degeneracy_in, points_in, eigvec_in, coupling, out, coords, degeneracy, points, eigvec, held, x, own, lattice, table, y, g, f, summed, coef, doubled, relayed, joined, partner, others, raw, joint_relayed, joint_g,
             load_sem, small_sem, lat_sem, relay_sem, side_sem, joint_send, joint_recv, x_send, x_recv, y_send, y_recv, f_send, f_recv):
    row, col, hi, core, lo = place()
    chip = row * 4 + col
    me = chip * 2 + core
    f32, bf16 = jnp.float32, jnp.bfloat16

    def plane_peer(d):
        r, c = (row + d[0]) % 4, (col + d[1]) % 4
        return r * 4 + c

    def peers():
        for c in (0, 1):
            for d in PLANE:
                yield plane_peer(d), c
        yield chip, 1 - core

    def plane_id(i, c):
        return ((i * 2 + hi) * 2 + c, lo)

    def z_id(z_hi, z_lo):
        return ((chip * 2 + z_hi) * 2 + core, z_lo)

    def iota(shape, dim):
        return lax.broadcasted_iota(jnp.int32, shape, dim)

    load = pltpu.make_async_copy(coupling, held, load_sem)
    small = [
        pltpu.make_async_copy(src, dst, small_sem.at[n])
        for n, (src, dst) in enumerate(
            ((coords_in, coords), (degeneracy_in, degeneracy), (points_in, points), (eigvec_in, eigvec))
        )
    ]
    for copy in small:
        copy.start()
    load.start()
    barrier = pltpu.get_barrier_semaphore()
    for i, c in peers():
        pl.semaphore_signal(barrier, inc=1, device_id=plane_id(i, c), device_id_type=MESH)
    for d in range(1, 8):
        z = (hi * 4 + lo + d) % 8
        pl.semaphore_signal(barrier, inc=1, device_id=z_id(z // 4, z % 4), device_id_type=MESH)

    pl.semaphore_wait(barrier, PEERS - 1 + 7)
    for copy in small:
        copy.wait()
    zeros = functools.partial(jnp.zeros, dtype=f32)
    stacked = jnp.concatenate(
        [coords[...].astype(f32), zeros((2, 16)), degeneracy[...].astype(f32), zeros((2, 16))], axis=0
    )
    spread16 = (iota((16, 128), 0) == iota((16, 128), 1) % 32 // 2).astype(f32)
    lat = jnp.dot(stacked, spread16, preferred_element_type=f32)
    line, lane = iota((8, 128), 0), iota((8, 128), 1)
    lat = lat + jnp.where(line == 3, 4 * (lane % 2), jnp.where(line == 4, 1, 0)).astype(f32)
    own[...] = jnp.where(lane // 32 == me % 4, lat, 0.0).astype(bf16)
    lattice[me] = own[...]

    for i, c in peers():
        pltpu.make_async_remote_copy(
            own, lattice.at[me], lat_sem.at[0], lat_sem.at[1],
            device_id=plane_id(i, c), device_id_type=MESH,
        ).start()
    pltpu.make_async_remote_copy(
        own, partner, side_sem.at[0], side_sem.at[1], device_id=z_id(1 - hi, lo), device_id_type=MESH
    ).start()
    load.wait()
    joint_p = (lo + STEP[0][JOINT]) % 4
    for n in range(2):
        pltpu.make_async_remote_copy(
            held.at[:, 3 * n + pick(WHICH, 1 - hi, JOINT), pl.ds(joint_p * 8, 8)], raw.at[n],
            side_sem.at[2], side_sem.at[3], device_id=z_id(1 - hi, lo), device_id_type=MESH,
        ).start()

    def piece(ref, i, c, unit):
        p = (lo + pick(STEP, c, unit)) % 4
        mode = (i // 8) * 3 + pick(WHICH, c, unit)
        return ref.at[:, mode, p * 8 + i % 8]

    def scatter(unit):
        for i, c in peers():
            pltpu.make_async_remote_copy(
                piece(held, i, c, unit), x.at[unit, me], x_send.at[unit], x_recv.at[unit],
                device_id=plane_id(i, c), device_id_type=MESH,
            ).start()

    for unit in range(EARLY):
        scatter(unit)

    def hand_on(source, n):
        def to(i):
            pltpu.make_async_remote_copy(
                source(i), joined.at[n, me], joint_send.at[n], joint_recv.at[n],
                device_id=plane_id(i, hi), device_id_type=MESH,
            ).start()

        for d in PLANE:
            to(plane_peer(d))
        pl.when(core != hi)(lambda: to(chip))

        @pl.when(core == hi)
        def keep():
            joined[n, me] = source(chip)[...]

    for unit in range(JOINT):
        x[unit, me] = piece(held, chip, core, unit)[...]

    def wait(ref, sem):
        pltpu.make_async_copy(ref, ref, sem).wait()

    grid = jnp.concatenate([points[...].astype(f32), zeros((5, 512))], axis=0)
    twice = []
    lane = iota((128, 256), 1)
    pair = (iota((128, 256), 0) == lane % 128 // 32 * 32 + lane // 128 * 16 + lane % 32 // 2).astype(f32)
    for n in range(4):
        twice.append(jnp.dot(grid[:, 128 * n : 128 * n + 128], pair, preferred_element_type=f32))
    line, lane = iota((8, 512), 0), iota((8, 512), 1)
    extra = jnp.where(line == 3, 1, jnp.where(line == 4, -4 * (lane % 2), 0)).astype(f32)
    for h in range(2):
        doubled[h] = jnp.concatenate([t[:, 128 * h : 128 * h + 128] for t in twice], axis=1) + extra
    rows16 = (iota((16, 8), 0) // 2 == iota((16, 8), 1)).astype(f32)
    columns = lax.dot_general(
        rows16, eigvec[...], (((1,), (1,)), ((), ())), precision=lax.Precision.HIGHEST, preferred_element_type=f32
    )
    for n in range(72):
        coef[n] = jnp.broadcast_to(columns[:, n : n + 1], (16, 128))

    wait(lattice.at[pl.ds(0, PEERS - 1)], lat_sem.at[1])
    def gathered(ref):
        groups = []
        for n in range(PEERS // 4):
            quad = ref[4 * n : 4 * n + 4].astype(f32)
            groups.append(quad[0] + quad[1] + quad[2] + quad[3])
        return jnp.concatenate(groups, axis=1)

    def tabulate(vectors, which, half):
        weights = 1.0 / vectors[5:6]
        vectors = vectors.astype(bf16)
        for n in range(2):
            turns = lax.dot_general(
                doubled.at[half][:, n * 256 : (n + 1) * 256], vectors,
                (((0,), (0,)), ((), ())), preferred_element_type=f32,
            )
            turns = turns - 16.0 * jnp.floor(turns * (1.0 / 16.0))
            w = jnp.abs(turns - 8.0) - 4.0
            s = w * w
            value = w * (((float(SINE[3]) * s + float(SINE[2])) * s + float(SINE[1])) * s + float(SINE[0]))
            table.at[which, half][n * 256 : (n + 1) * 256, :] = (value * weights).astype(bf16)

    def send(unit, half):
        p = (lo + pick(STEP, core, unit)) % 4
        pltpu.make_async_remote_copy(
            y.at[unit, half], g.at[unit, hi], y_send.at[unit, half], y_recv.at[unit, hi],
            device_id=z_id(half, p), device_id_type=MESH,
        ).start()

    def contract(unit, half, target):
        part = jnp.dot(table[0, half], x.at[unit].reshape(1024, 128)[...], preferred_element_type=f32)
        target[...] = part.astype(bf16).reshape(PEERS, 16, 128)

    def transform(unit):
        wait(x.at[unit, pl.ds(0, PEERS - 1)], x_recv.at[unit])
        if unit in LATE:
            n = LATE.index(unit)
            for half in (0, 1):
                contract(unit, half, y.at[unit, half])
            for i, c in peers():
                pltpu.make_async_remote_copy(
                    y.at[unit, :, i * 2 + c], relayed.at[n, :, me], relay_sem.at[0, n], relay_sem.at[1, n],
                    device_id=plane_id(i, c), device_id_type=MESH,
                ).start()
            relayed[n, :, me] = y[unit, :, me]
            return
        contract(unit, 1 - hi, y.at[unit, 1 - hi])
        send(unit, 1 - hi)
        if unit == 0:
            forward_lattice()
            for later in range(EARLY, JOINT):
                scatter(later)
            hand_on(lambda i: piece(held, i, hi, JOINT), 0)
            tabulate(vectors, 0, hi)
            contract(unit, hi, g.at[unit, hi])
        elif unit == 1:
            contract(unit, hi, y.at[unit, hi])

            @pl.when(core == 0)
            def keep():
                g[unit, hi] = y[unit, hi]

            pl.when(core == 1)(lambda: send(unit, hi))
        else:
            contract(unit, hi, y.at[unit, hi])
            send(unit, hi)

    vectors = gathered(lattice)
    tabulate(vectors, 0, 1 - hi)

    def forward_lattice():
        wait(partner, side_sem.at[1])
        for i, c in peers():
            pltpu.make_async_remote_copy(
                partner, others.at[me], side_sem.at[4], side_sem.at[5],
                device_id=plane_id(i, c), device_id_type=MESH,
            ).start()
        others[me] = partner[...]

    def forward_raw():
        wait(raw, side_sem.at[3])
        hand_on(lambda i: raw.at[i // 8, :, i % 8], 1)

    def tabulate_others():
        wait(others.at[pl.ds(0, PEERS - 1)], side_sem.at[5])

        @pl.when(core == hi)
        def active():
            vectors = gathered(others)
            for half in (0, 1):
                tabulate(vectors, 1, half)

    def transform_joint():
        @pl.when(core == hi)
        def active():
            for n in range(2):
                wait(x.at[0, pl.ds(0, PEERS - 1)], joint_recv.at[n])
            for half in (0, 1):
                part = sum(
                    jnp.dot(table[n, half], joined.at[n].reshape(1024, 128)[...], preferred_element_type=f32)
                    for n in range(2)
                )
                y[JOINT, half] = part.astype(bf16).reshape(PEERS, 16, 128)
            for i, c in peers():
                pltpu.make_async_remote_copy(
                    y.at[JOINT, :, i * 2 + c], joint_relayed.at[:, chip], relay_sem.at[0, 2], relay_sem.at[1, 2],
                    device_id=plane_id(i, c), device_id_type=MESH,
                ).start()
            joint_relayed[:, chip] = y[JOINT, :, me]

    def relay_joint():
        pl.when(core == hi)(lambda: wait(x.at[0, pl.ds(0, 15)], relay_sem.at[1, 2]))
        pl.when(core != hi)(lambda: wait(x.at[0, pl.ds(0, 16)], relay_sem.at[1, 2]))
        for half in (0, 1):
            pltpu.make_async_remote_copy(
                joint_relayed.at[half], joint_g.at[hi], y_send.at[JOINT, half], y_recv.at[JOINT, hi],
                device_id=z_id(half, joint_p), device_id_type=MESH,
            ).start()

    def relay(unit):
        n = LATE.index(unit)
        wait(x.at[0, pl.ds(0, PEERS - 1)], relay_sem.at[1, n])
        for half in (0, 1):
            pltpu.make_async_remote_copy(
                relayed.at[n, half], g.at[unit, hi], y_send.at[unit, half], y_recv.at[unit, hi],
                device_id=z_id(half, (lo + STEP[0][unit]) % 4), device_id_type=MESH,
            ).start()

    def spread(unit):
        wait(g.at[unit, 1 - hi], y_recv.at[unit, 1 - hi])
        if unit == 1:
            pl.when(core == 1)(lambda: wait(g.at[unit, hi], y_recv.at[unit, hi]))
        elif unit > 1:
            wait(g.at[unit, hi], y_recv.at[unit, hi])
        total = g[unit, 0].astype(f32) + g[unit, 1].astype(f32)
        f[unit * PEERS : (unit + 1) * PEERS] = total.astype(bf16)
        step = pick(STEP, core, unit)
        mode = (chip // 8) * 3 + pick(WHICH, core, unit)
        place_of = summed.at[step, mode, chip % 8]
        for i, c in peers():
            pltpu.make_async_remote_copy(
                f.at[unit * PEERS + i * 2 + c], place_of, f_send.at[unit], f_recv.at[step],
                device_id=plane_id(i, c), device_id_type=MESH,
            ).start()
        place_of[...] = f[unit * PEERS + me]

    odd = iota((16, 128), 0) % 2 == 1

    def rotate(step):
        made = [STEP[c][: LATE[0]].count(step) for c in (0, 1)]
        for c in (0, 1):
            pl.when(core == c)(lambda: wait(f.at[pl.ds(0, 16 * sum(made) - made[c])], f_recv.at[step]))
        for unit in LATE:
            if step == STEP[0][unit]:
                for half in (0, 1):
                    wait(joint_g.at[half] if unit == JOINT else g.at[unit, half], y_recv.at[unit, half])
        re = (lo + 4 - step) % 4

        def block(b, _):
            def value(k):
                for unit in LATE:
                    for c in (0, 1):
                        if STEP[c][unit] == step and WHICH[c][unit] == k % 3:
                            if unit == JOINT:
                                return joint_g[c, k // 3 * 8 + b].astype(f32)
                            n = (k // 3 * 8 + b) * 2 + c
                            return g[unit, 0, n].astype(f32) + g[unit, 1, n].astype(f32)
                return summed[step, k, b].astype(f32)

            plain = [value(k) for k in range(6)]
            turned = [jnp.where(odd, pltpu.roll(v, 1, 0), -pltpu.roll(v, 15, 0)) for v in plain]
            for n in range(6):
                total = None
                for k in range(6):
                    at = (k * 6 + n) * 2
                    term = coef[at] * plain[k] + coef[at + 1] * turned[k]
                    total = term if total is None else total + term
                out[:, re, n, b] = total.reshape(8, 2, 128)
            return 0

        lax.fori_loop(0, 8, block, 0)

    transform(0)
    transform(1)
    forward_raw()
    transform(2)
    transform(3)
    transform(4)
    tabulate_others()
    transform_joint()
    spread(0)
    relay(3)
    spread(1)
    relay(4)
    relay_joint()
    spread(2)
    wait(lattice.at[pl.ds(0, PEERS - 1)], lat_sem.at[0])
    for n in range(2):
        wait(x.at[0, pl.ds(0, PEERS - 1)], relay_sem.at[0, n])
    pl.when(core == hi)(lambda: wait(x.at[0, pl.ds(0, PEERS - 1)], relay_sem.at[0, 2]))
    wait(partner, side_sem.at[0])
    wait(raw, side_sem.at[2])
    wait(others.at[pl.ds(0, PEERS - 1)], side_sem.at[4])
    for n in range(2):
        pl.when(core == hi)(lambda: wait(x.at[0, pl.ds(0, 15)], joint_send.at[n]))
        pl.when(core != hi)(lambda: wait(x.at[0, pl.ds(0, 16)], joint_send.at[n]))
    for unit in range(JOINT):
        wait(x.at[unit, pl.ds(0, PEERS - 1)], x_send.at[unit])
    rotate(0)
    for unit in range(LATE[0]):
        wait(f.at[pl.ds(0, PEERS - 1)], f_send.at[unit])
        wait(g.at[unit, 0], y_send.at[unit, 1 - hi])
        if unit == 1:
            pl.when(core == 1)(lambda: wait(g.at[unit, 0], y_send.at[unit, hi]))
        elif unit > 1:
            wait(g.at[unit, 0], y_send.at[unit, hi])
    rotate(3)
    rotate(1)
    rotate(2)
    for half in (0, 1):
        for unit in LATE[:2]:
            wait(g.at[unit, 0], y_send.at[unit, half])
        wait(joint_g.at[0], y_send.at[JOINT, half])


def per_device(coupling, rp_coords, degeneracy, qpoints, eigvec):
    blocks = coupling.reshape(16, 2, 6, 32, 128).transpose(0, 2, 3, 1, 4)
    vectors = eigvec.transpose(2, 3, 1, 0).reshape(72, 8)
    vmem = pl.BlockSpec(memory_space=pltpu.VMEM)
    dma = pltpu.SemaphoreType.DMA
    bf = jnp.bfloat16
    mixed = pl.pallas_call(
        exchange,
        out_shape=jax.ShapeDtypeStruct((8, 4, 6, 8, 2, 128), jnp.float32),
        in_specs=[pl.BlockSpec(memory_space=pl.ANY)] * 5,
        out_specs=vmem,
        scratch_shapes=[
            pltpu.VMEM((3, 16), jnp.int32),
            pltpu.VMEM((1, 16), jnp.int32),
            pltpu.VMEM((3, 512), jnp.int32),
            pltpu.VMEM((72, 8), jnp.float32),
            pltpu.VMEM((16, 6, 32, 2, 128), bf),
            pltpu.VMEM((JOINT, PEERS, 16, 2, 128), bf),
            pltpu.VMEM((8, 128), bf),
            pltpu.VMEM((PEERS, 8, 128), bf),
            pltpu.VMEM((2, 2, 512, 1024), bf),
            pltpu.VMEM((UNITS, 2, PEERS, 16, 128), bf),
            pltpu.VMEM((UNITS, 2, PEERS, 16, 128), bf),
            pltpu.VMEM((UNITS * PEERS, 16, 128), bf),
            pltpu.VMEM((4, 6, 8, 16, 128), bf),
            pltpu.VMEM((72, 16, 128), jnp.float32),
            pltpu.VMEM((2, 8, 512), jnp.float32),
            pltpu.VMEM((2, 2, PEERS, 16, 128), bf),
            pltpu.VMEM((2, PEERS, 16, 2, 128), bf),
            pltpu.VMEM((8, 128), bf),
            pltpu.VMEM((PEERS, 8, 128), bf),
            pltpu.VMEM((2, 16, 8, 2, 128), bf),
            pltpu.VMEM((2, 16, 16, 128), bf),
            pltpu.VMEM((2, 16, 16, 128), bf),
            dma, dma((4,)), dma((2,)), dma((2, 3)), dma((6,)), dma((2,)), dma((2,)), dma((UNITS,)), dma((UNITS,)),
            dma((UNITS, 2)), dma((UNITS, 2)), dma((UNITS,)), dma((4,)),
        ],
        compiler_params=pltpu.CompilerParams(
            collective_id=0, has_side_effects=True, vmem_limit_bytes=40 * 2**20
        ),
        name="exchange",
    )(*(pltpu.with_memory_space_constraint(v, pltpu.HBM) for v in (rp_coords, degeneracy.reshape(1, 16), qpoints, vectors, blocks)))
    return mixed.transpose(0, 1, 4, 2, 3, 5).reshape(8, 4, 2, 6, 1024)


def solution(mesh):
    return jax.shard_map(
        per_device,
        mesh=mesh,
        in_specs=(
            P("rp", "re", None, None, None),
            P(None, "rp"),
            P("rp"),
            P(),
            P("rp", None, None, None),
        ),
        out_specs=P("rp", None, None, None, "re"),
        check_vma=False,
    )
```

```python
import functools
import math

import numpy as np

import jax
import jax.numpy as jnp
from jax import lax
from jax.experimental import pallas as pl
from jax.experimental.pallas import tpu as pltpu
from jax.sharding import PartitionSpec as P

MESH = pl.DeviceIdType.MESH
UNITS = 6
PEERS = 32
LATE = (3, 4, 5)
JOINT = 5
EARLY = 3
STEP = ((0, 0, 2, 3, 1, 2), (0, 3, 1, 3, 1, 2))
WHICH = ((0, 2, 0, 0, 0, 2), (1, 2, 2, 1, 1, 1))
PLANE = ((2, 2), (2, 1), (1, 2), (2, 3), (3, 2), (1, 1), (3, 3), (1, 3), (3, 1), (2, 0), (0, 2), (0, 1), (1, 0), (0, 3), (3, 0))
SINE = np.linalg.solve(
    np.array([[w ** (2 * i + 1) for i in range(4)] for w in (1.0, 2.0, 3.0, 4.0)]),
    np.sin(np.pi / 8 * np.arange(1, 5)),
)


def place():
    rp, lo = lax.axis_index("rp"), lax.axis_index("re")
    return rp // 16, (rp // 4) % 4, (rp // 2) % 2, rp % 2, lo


def pick(table, core, unit):
    if isinstance(core, int):
        return table[core][unit]
    return jnp.where(core == 0, table[0][unit], table[1][unit])


def exchange(coords_in, degeneracy_in, points_in, eigvec_in, coupling, out, coords, degeneracy, points, eigvec, held, x, own, lattice, table, y, g, f, summed, coef, doubled, relayed, joined, partner, raw, joint_relayed, joint_g,
             load_sem, small_sem, lat_send, lat_recv, raw_sem, joint_sem, relay_send, relay_recv,
             x_send, x_recv, y_send, y_recv, f_send, f_recv):
    row, col, hi, core, lo = place()
    chip = row * 4 + col
    me = chip * 2 + core
    f32, bf16 = jnp.float32, jnp.bfloat16

    def plane_peer(d):
        r, c = (row + d[0]) % 4, (col + d[1]) % 4
        return r * 4 + c

    def peers():
        for c in (0, 1):
            for d in PLANE:
                yield plane_peer(d), c
        yield chip, 1 - core

    def plane_id(i, c):
        return ((i * 2 + hi) * 2 + c, lo)

    def z_id(z_hi, z_lo):
        return ((chip * 2 + z_hi) * 2 + core, z_lo)

    def iota(shape, dim):
        return lax.broadcasted_iota(jnp.int32, shape, dim)

    load = pltpu.make_async_copy(coupling, held, load_sem)
    small = [
        pltpu.make_async_copy(src, dst, small_sem.at[n])
        for n, (src, dst) in enumerate(
            ((coords_in, coords), (degeneracy_in, degeneracy), (points_in, points), (eigvec_in, eigvec))
        )
    ]
    for copy in small:
        copy.start()
    load.start()
    barrier = pltpu.get_barrier_semaphore()
    for i, c in peers():
        pl.semaphore_signal(barrier, inc=1, device_id=plane_id(i, c), device_id_type=MESH)
    for d in range(1, 8):
        z = (hi * 4 + lo + d) % 8
        pl.semaphore_signal(barrier, inc=1, device_id=z_id(z // 4, z % 4), device_id_type=MESH)

    pl.semaphore_wait(barrier, PEERS - 1 + 7)
    for copy in small:
        copy.wait()
    zeros = functools.partial(jnp.zeros, dtype=f32)
    stacked = jnp.concatenate(
        [coords[...].astype(f32), zeros((2, 16)), degeneracy[...].astype(f32), zeros((2, 16))], axis=0
    )
    spread16 = (iota((16, 128), 0) == iota((16, 128), 1) % 32 // 2).astype(f32)
    lat = jnp.dot(stacked, spread16, preferred_element_type=f32)
    line, lane = iota((8, 128), 0), iota((8, 128), 1)
    lat = lat + jnp.where(line == 3, 4 * (lane % 2), jnp.where(line == 4, 1, 0)).astype(f32)
    own[...] = jnp.where(lane // 32 == me % 4, lat, 0.0).astype(bf16)
    lattice[me] = own[...]

    pltpu.make_async_remote_copy(
        own, partner, lat_send, lat_recv.at[1], device_id=z_id(1 - hi, lo), device_id_type=MESH
    ).start()
    load.wait()
    joint_p = (lo + STEP[0][JOINT]) % 4
    for n in range(2):
        pltpu.make_async_remote_copy(
            held.at[:, 3 * n + pick(WHICH, 1 - hi, JOINT), pl.ds(joint_p * 8, 8)], raw.at[n],
            raw_sem.at[0], raw_sem.at[1], device_id=z_id(1 - hi, lo), device_id_type=MESH,
        ).start()

    for i, c in peers():
        pltpu.make_async_remote_copy(
            own, lattice.at[me], lat_send, lat_recv.at[0],
            device_id=plane_id(i, c), device_id_type=MESH,
        ).start()
    def piece(ref, i, c, unit):
        p = (lo + pick(STEP, c, unit)) % 4
        mode = (i // 8) * 3 + pick(WHICH, c, unit)
        return ref.at[:, mode, p * 8 + i % 8]

    def scatter(unit):
        for i, c in peers():
            pltpu.make_async_remote_copy(
                piece(held, i, c, unit), x.at[unit, me], x_send, x_recv.at[unit],
                device_id=plane_id(i, c), device_id_type=MESH,
            ).start()

    for unit in range(EARLY):
        scatter(unit)

    def hand_on(source, n):
        def to(i):
            pltpu.make_async_remote_copy(
                source(i), joined.at[n, me], joint_sem.at[0], joint_sem.at[1],
                device_id=plane_id(i, hi), device_id_type=MESH,
            ).start()

        for d in PLANE:
            to(plane_peer(d))
        pl.when(core != hi)(lambda: to(chip))

        @pl.when(core == hi)
        def keep():
            joined[n, me] = source(chip)[...]

    for unit in range(JOINT):
        x[unit, me] = piece(held, chip, core, unit)[...]

    def wait(ref, sem):
        pltpu.make_async_copy(ref, ref, sem).wait()

    grid = jnp.concatenate([points[...].astype(f32), zeros((5, 512))], axis=0)
    twice = []
    lane = iota((128, 256), 1)
    pair = (iota((128, 256), 0) == lane % 128 // 32 * 32 + lane // 128 * 16 + lane % 32 // 2).astype(f32)
    for n in range(4):
        twice.append(jnp.dot(grid[:, 128 * n : 128 * n + 128], pair, preferred_element_type=f32))
    line, lane = iota((8, 512), 0), iota((8, 512), 1)
    extra = jnp.where(line == 3, 1, jnp.where(line == 4, -4 * (lane % 2), 0)).astype(f32)
    for h in range(2):
        doubled[h] = jnp.concatenate([t[:, 128 * h : 128 * h + 128] for t in twice], axis=1) + extra
    rows16 = (iota((16, 8), 0) // 2 == iota((16, 8), 1)).astype(f32)
    columns = lax.dot_general(
        rows16, eigvec[...], (((1,), (1,)), ((), ())), precision=lax.Precision.HIGHEST, preferred_element_type=f32
    )
    for n in range(72):
        coef[n] = jnp.broadcast_to(columns[:, n : n + 1], (16, 128))

    wait(lattice.at[pl.ds(0, PEERS - 1)], lat_recv.at[0])
    def gathered(first):
        groups = []
        for n in range(PEERS // 4):
            quad = lattice[first + 4 * n : first + 4 * n + 4].astype(f32)
            groups.append(quad[0] + quad[1] + quad[2] + quad[3])
        return jnp.concatenate(groups, axis=1)

    def tabulate(vectors, which, half):
        weights = 1.0 / vectors[5:6]
        vectors = vectors.astype(bf16)
        for n in range(2):
            turns = lax.dot_general(
                doubled.at[half][:, n * 256 : (n + 1) * 256], vectors,
                (((0,), (0,)), ((), ())), preferred_element_type=f32,
            )
            turns = turns - 16.0 * jnp.floor(turns * (1.0 / 16.0))
            w = jnp.abs(turns - 8.0) - 4.0
            s = w * w
            value = w * (((float(SINE[3]) * s + float(SINE[2])) * s + float(SINE[1])) * s + float(SINE[0]))
            table.at[which, half][n * 256 : (n + 1) * 256, :] = (value * weights).astype(bf16)

    def send(unit, half):
        p = (lo + pick(STEP, core, unit)) % 4
        pltpu.make_async_remote_copy(
            y.at[unit, half], g.at[unit, hi], y_send, y_recv.at[unit],
            device_id=z_id(half, p), device_id_type=MESH,
        ).start()

    def contract(unit, half, target):
        part = jnp.dot(table[0, half], x.at[unit].reshape(1024, 128)[...], preferred_element_type=f32)
        target[...] = part.astype(bf16).reshape(PEERS, 16, 128)

    def transform(unit):
        wait(x.at[unit, pl.ds(0, PEERS - 1)], x_recv.at[unit])
        if unit in LATE:
            n = LATE.index(unit)
            for half in (0, 1):
                contract(unit, half, y.at[unit, half])
            for i, c in peers():
                pltpu.make_async_remote_copy(
                    y.at[unit, :, i * 2 + c], relayed.at[n, :, me], relay_send, relay_recv.at[n],
                    device_id=plane_id(i, c), device_id_type=MESH,
                ).start()
            relayed[n, :, me] = y[unit, :, me]
            return
        contract(unit, 1 - hi, y.at[unit, 1 - hi])
        send(unit, 1 - hi)
        if unit == 0:
            forward_lattice()
            for later in range(EARLY, JOINT):
                scatter(later)
            hand_on(lambda i: piece(held, i, hi, JOINT), 0)
            tabulate(vectors, 0, hi)
            contract(unit, hi, g.at[unit, hi])
        elif unit == 1:
            contract(unit, hi, y.at[unit, hi])

            @pl.when(core == 0)
            def keep():
                g[unit, hi] = y[unit, hi]

            pl.when(core == 1)(lambda: send(unit, hi))
        else:
            contract(unit, hi, y.at[unit, hi])
            send(unit, hi)

    vectors = gathered(0)
    tabulate(vectors, 0, 1 - hi)

    def forward_lattice():
        wait(partner, lat_recv.at[1])
        for i, c in peers():
            pltpu.make_async_remote_copy(
                partner, lattice.at[PEERS + me], lat_send, lat_recv.at[2],
                device_id=plane_id(i, c), device_id_type=MESH,
            ).start()
        lattice[PEERS + me] = partner[...]

    def forward_raw():
        wait(raw, raw_sem.at[1])
        hand_on(lambda i: raw.at[i // 8, :, i % 8], 1)

    def tabulate_others():
        wait(lattice.at[pl.ds(0, PEERS - 1)], lat_recv.at[2])

        @pl.when(core == hi)
        def active():
            vectors = gathered(PEERS)
            for half in (0, 1):
                tabulate(vectors, 1, half)

    def transform_joint():
        @pl.when(core == hi)
        def active():
            wait(x.at[pl.ds(0, 2), pl.ds(0, PEERS - 1)], joint_sem.at[1])
            for half in (0, 1):
                part = sum(
                    jnp.dot(table[n, half], joined.at[n].reshape(1024, 128)[...], preferred_element_type=f32)
                    for n in range(2)
                )
                y[JOINT, half] = part.astype(bf16).reshape(PEERS, 16, 128)
            for i, c in peers():
                pltpu.make_async_remote_copy(
                    y.at[JOINT, :, i * 2 + c], joint_relayed.at[:, chip], relay_send, relay_recv.at[2],
                    device_id=plane_id(i, c), device_id_type=MESH,
                ).start()
            joint_relayed[:, chip] = y[JOINT, :, me]

    def relay_joint():
        pl.when(core == hi)(lambda: wait(x.at[0, pl.ds(0, 15)], relay_recv.at[2]))
        pl.when(core != hi)(lambda: wait(x.at[0, pl.ds(0, 16)], relay_recv.at[2]))
        for half in (0, 1):
            pltpu.make_async_remote_copy(
                joint_relayed.at[half], joint_g.at[hi], y_send, y_recv.at[JOINT],
                device_id=z_id(half, joint_p), device_id_type=MESH,
            ).start()

    def relay(unit):
        n = LATE.index(unit)
        wait(x.at[0, pl.ds(0, PEERS - 1)], relay_recv.at[n])
        for half in (0, 1):
            pltpu.make_async_remote_copy(
                relayed.at[n, half], g.at[unit, hi], y_send, y_recv.at[unit],
                device_id=z_id(half, (lo + STEP[0][unit]) % 4), device_id_type=MESH,
            ).start()

    def spread(unit):
        if unit == 0:
            wait(g.at[unit, 0], y_recv.at[unit])
        elif unit == 1:
            pl.when(core == 0)(lambda: wait(g.at[unit, 0], y_recv.at[unit]))
            pl.when(core == 1)(lambda: wait(g.at[unit], y_recv.at[unit]))
        else:
            wait(g.at[unit], y_recv.at[unit])
        total = g[unit, 0].astype(f32) + g[unit, 1].astype(f32)
        f[unit * PEERS : (unit + 1) * PEERS] = total.astype(bf16)
        step = pick(STEP, core, unit)
        mode = (chip // 8) * 3 + pick(WHICH, core, unit)
        place_of = summed.at[step, mode, chip % 8]
        for i, c in peers():
            pltpu.make_async_remote_copy(
                f.at[unit * PEERS + i * 2 + c], place_of, f_send, f_recv.at[step],
                device_id=plane_id(i, c), device_id_type=MESH,
            ).start()
        place_of[...] = f[unit * PEERS + me]

    odd = iota((16, 128), 0) % 2 == 1

    def rotate(step):
        made = [STEP[c][: LATE[0]].count(step) for c in (0, 1)]
        for c in (0, 1):
            pl.when(core == c)(lambda: wait(f.at[pl.ds(0, 16 * sum(made) - made[c])], f_recv.at[step]))
        for unit in LATE:
            if step == STEP[0][unit]:
                wait(joint_g if unit == JOINT else g.at[unit], y_recv.at[unit])
        re = (lo + 4 - step) % 4

        def block(b, _):
            def value(k):
                for unit in LATE:
                    for c in (0, 1):
                        if STEP[c][unit] == step and WHICH[c][unit] == k % 3:
                            if unit == JOINT:
                                return joint_g[c, k // 3 * 8 + b].astype(f32)
                            n = (k // 3 * 8 + b) * 2 + c
                            return g[unit, 0, n].astype(f32) + g[unit, 1, n].astype(f32)
                return summed[step, k, b].astype(f32)

            plain = [value(k) for k in range(6)]
            turned = [jnp.where(odd, pltpu.roll(v, 1, 0), -pltpu.roll(v, 15, 0)) for v in plain]
            for n in range(6):
                total = None
                for k in range(6):
                    at = (k * 6 + n) * 2
                    term = coef[at] * plain[k] + coef[at + 1] * turned[k]
                    total = term if total is None else total + term
                out[:, re, n, b] = total.reshape(8, 2, 128)
            return 0

        lax.fori_loop(0, 8, block, 0)

    transform(0)
    transform(1)
    forward_raw()
    transform(2)
    transform(3)
    transform(4)
    tabulate_others()
    transform_joint()
    spread(0)
    relay(3)
    spread(1)
    relay(4)
    relay_joint()
    spread(2)
    wait(lattice.at[pl.ds(0, 2 * PEERS - 1)], lat_send)
    wait(raw, raw_sem.at[0])
    wait(x.at[:, pl.ds(0, PEERS - 1)], x_send)
    pl.when(core == hi)(lambda: wait(x.at[pl.ds(0, 2), pl.ds(0, 15)], joint_sem.at[0]))
    pl.when(core != hi)(lambda: wait(x.at[pl.ds(0, 2), pl.ds(0, 16)], joint_sem.at[0]))
    pl.when(core == hi)(lambda: wait(x.at[pl.ds(0, 3), pl.ds(0, PEERS - 1)], relay_send))
    pl.when(core != hi)(lambda: wait(x.at[pl.ds(0, 2), pl.ds(0, PEERS - 1)], relay_send))
    rotate(0)
    wait(f.at[pl.ds(0, LATE[0] * (PEERS - 1))], f_send)
    rotate(3)
    rotate(1)
    rotate(2)
    halves = g.reshape(2 * UNITS, PEERS, 16, 128)
    pl.when(core == 0)(lambda: wait(halves.at[pl.ds(0, 9)], y_send))
    pl.when(core == 1)(lambda: wait(halves.at[pl.ds(0, 10)], y_send))


def per_device(coupling, rp_coords, degeneracy, qpoints, eigvec):
    blocks = coupling.reshape(16, 2, 6, 32, 128).transpose(0, 2, 3, 1, 4)
    vectors = eigvec.transpose(2, 3, 1, 0).reshape(72, 8)
    vmem = pl.BlockSpec(memory_space=pltpu.VMEM)
    dma = pltpu.SemaphoreType.DMA
    bf = jnp.bfloat16
    mixed = pl.pallas_call(
        exchange,
        out_shape=jax.ShapeDtypeStruct((8, 4, 6, 8, 2, 128), jnp.float32),
        in_specs=[pl.BlockSpec(memory_space=pl.ANY)] * 5,
        out_specs=vmem,
        scratch_shapes=[
            pltpu.VMEM((3, 16), jnp.int32),
            pltpu.VMEM((1, 16), jnp.int32),
            pltpu.VMEM((3, 512), jnp.int32),
            pltpu.VMEM((72, 8), jnp.float32),
            pltpu.VMEM((16, 6, 32, 2, 128), bf),
            pltpu.VMEM((JOINT, PEERS, 16, 2, 128), bf),
            pltpu.VMEM((8, 128), bf),
            pltpu.VMEM((2 * PEERS, 8, 128), bf),
            pltpu.VMEM((2, 2, 512, 1024), bf),
            pltpu.VMEM((UNITS, 2, PEERS, 16, 128), bf),
            pltpu.VMEM((UNITS, 2, PEERS, 16, 128), bf),
            pltpu.VMEM((UNITS * PEERS, 16, 128), bf),
            pltpu.VMEM((4, 6, 8, 16, 128), bf),
            pltpu.VMEM((72, 16, 128), jnp.float32),
            pltpu.VMEM((2, 8, 512), jnp.float32),
            pltpu.VMEM((2, 2, PEERS, 16, 128), bf),
            pltpu.VMEM((2, PEERS, 16, 2, 128), bf),
            pltpu.VMEM((8, 128), bf),
            pltpu.VMEM((2, 16, 8, 2, 128), bf),
            pltpu.VMEM((2, 16, 16, 128), bf),
            pltpu.VMEM((2, 16, 16, 128), bf),
            dma, dma((4,)), dma, dma((3,)), dma((2,)), dma((2,)), dma, dma((3,)),
            dma, dma((JOINT,)), dma, dma((UNITS,)), dma, dma((4,)),
        ],
        compiler_params=pltpu.CompilerParams(
            collective_id=0, has_side_effects=True, vmem_limit_bytes=40 * 2**20
        ),
        name="exchange",
    )(*(pltpu.with_memory_space_constraint(v, pltpu.HBM) for v in (rp_coords, degeneracy.reshape(1, 16), qpoints, vectors, blocks)))
    return mixed.transpose(0, 1, 4, 2, 3, 5).reshape(8, 4, 2, 6, 1024)


def solution(mesh):
    return jax.shard_map(
        per_device,
        mesh=mesh,
        in_specs=(
            P("rp", "re", None, None, None),
            P(None, "rp"),
            P("rp"),
            P(),
            P("rp", None, None, None),
        ),
        out_specs=P("rp", None, None, None, "re"),
        check_vma=False,
    )
```

```python
import functools
import math

import numpy as np

import jax
import jax.numpy as jnp
from jax import lax
from jax.experimental import pallas as pl
from jax.experimental.pallas import tpu as pltpu
from jax.sharding import PartitionSpec as P

MESH = pl.DeviceIdType.MESH
UNITS = 6
PEERS = 32
LATE = (3, 4, 5)
JOINT = 5
EARLY = 3
STEP = ((0, 0, 2, 3, 1, 2), (0, 3, 1, 3, 1, 2))
WHICH = ((0, 2, 0, 0, 0, 2), (1, 2, 2, 1, 1, 1))
PLANE = ((2, 2), (2, 1), (1, 2), (2, 3), (3, 2), (1, 1), (3, 3), (1, 3), (3, 1), (2, 0), (0, 2), (0, 1), (1, 0), (0, 3), (3, 0))
SINE = np.linalg.solve(
    np.array([[w ** (2 * i + 1) for i in range(4)] for w in (1.0, 2.0, 3.0, 4.0)]),
    np.sin(np.pi / 8 * np.arange(1, 5)),
)


def place():
    rp, lo = lax.axis_index("rp"), lax.axis_index("re")
    return rp // 16, (rp // 4) % 4, (rp // 2) % 2, rp % 2, lo


def pick(table, core, unit):
    if isinstance(core, int):
        return table[core][unit]
    return jnp.where(core == 0, table[0][unit], table[1][unit])


def exchange(coords_in, degeneracy_in, points_in, eigvec_in, coupling, out, coords, degeneracy, points, eigvec, held, x, own, lattice, table, y, g, f, summed, coef, doubled, relayed, joined, partner, raw, joint_relayed, joint_g, so_far,
             load_sem, small_sem, lat_send, lat_recv, raw_sem, joint_sem, relay_send, relay_recv,
             x_send, x_recv, y_send, y_recv, f_send, f_recv):
    row, col, hi, core, lo = place()
    chip = row * 4 + col
    me = chip * 2 + core
    f32, bf16 = jnp.float32, jnp.bfloat16

    def plane_peer(d):
        r, c = (row + d[0]) % 4, (col + d[1]) % 4
        return r * 4 + c

    def peers():
        for c in (0, 1):
            for d in PLANE:
                yield plane_peer(d), c
        yield chip, 1 - core

    def plane_id(i, c):
        return ((i * 2 + hi) * 2 + c, lo)

    def z_id(z_hi, z_lo):
        return ((chip * 2 + z_hi) * 2 + core, z_lo)

    def iota(shape, dim):
        return lax.broadcasted_iota(jnp.int32, shape, dim)

    load = pltpu.make_async_copy(coupling, held, load_sem)
    small = [
        pltpu.make_async_copy(src, dst, small_sem.at[n])
        for n, (src, dst) in enumerate(
            ((coords_in, coords), (degeneracy_in, degeneracy), (points_in, points), (eigvec_in, eigvec))
        )
    ]
    for copy in small:
        copy.start()
    load.start()
    barrier = pltpu.get_barrier_semaphore()
    for i, c in peers():
        pl.semaphore_signal(barrier, inc=1, device_id=plane_id(i, c), device_id_type=MESH)
    for d in range(1, 8):
        z = (hi * 4 + lo + d) % 8
        pl.semaphore_signal(barrier, inc=1, device_id=z_id(z // 4, z % 4), device_id_type=MESH)

    pl.semaphore_wait(barrier, PEERS - 1 + 7)
    for copy in small:
        copy.wait()
    zeros = functools.partial(jnp.zeros, dtype=f32)
    stacked = jnp.concatenate(
        [coords[...].astype(f32), zeros((2, 16)), degeneracy[...].astype(f32), zeros((2, 16))], axis=0
    )
    spread16 = (iota((16, 128), 0) == iota((16, 128), 1) % 32 // 2).astype(f32)
    lat = jnp.dot(stacked, spread16, preferred_element_type=f32)
    line, lane = iota((8, 128), 0), iota((8, 128), 1)
    lat = lat + jnp.where(line == 3, 4 * (lane % 2), jnp.where(line == 4, 1, 0)).astype(f32)
    own[...] = jnp.where(lane // 32 == me % 4, lat, 0.0).astype(bf16)
    lattice[me] = own[...]

    pltpu.make_async_remote_copy(
        own, partner, lat_send, lat_recv.at[1], device_id=z_id(1 - hi, lo), device_id_type=MESH
    ).start()
    load.wait()
    joint_p = (lo + STEP[0][JOINT]) % 4
    for n in range(2):
        pltpu.make_async_remote_copy(
            held.at[:, 3 * n + pick(WHICH, 1 - hi, JOINT), pl.ds(joint_p * 8, 8)], raw.at[n],
            raw_sem.at[0], raw_sem.at[1], device_id=z_id(1 - hi, lo), device_id_type=MESH,
        ).start()

    for i, c in peers():
        pltpu.make_async_remote_copy(
            own, lattice.at[me], lat_send, lat_recv.at[0],
            device_id=plane_id(i, c), device_id_type=MESH,
        ).start()
    def piece(ref, i, c, unit):
        p = (lo + pick(STEP, c, unit)) % 4
        mode = (i // 8) * 3 + pick(WHICH, c, unit)
        return ref.at[:, mode, p * 8 + i % 8]

    def scatter(unit):
        for i, c in peers():
            pltpu.make_async_remote_copy(
                piece(held, i, c, unit), x.at[unit, me], x_send, x_recv.at[unit],
                device_id=plane_id(i, c), device_id_type=MESH,
            ).start()

    for unit in range(EARLY):
        scatter(unit)

    def hand_on(source, n):
        def to(i):
            pltpu.make_async_remote_copy(
                source(i), joined.at[n, me], joint_sem.at[0], joint_sem.at[1],
                device_id=plane_id(i, hi), device_id_type=MESH,
            ).start()

        for d in PLANE:
            to(plane_peer(d))
        pl.when(core != hi)(lambda: to(chip))

        @pl.when(core == hi)
        def keep():
            joined[n, me] = source(chip)[...]

    for unit in range(JOINT):
        x[unit, me] = piece(held, chip, core, unit)[...]

    def wait(ref, sem):
        pltpu.make_async_copy(ref, ref, sem).wait()

    grid = jnp.concatenate([points[...].astype(f32), zeros((5, 512))], axis=0)
    twice = []
    lane = iota((128, 256), 1)
    pair = (iota((128, 256), 0) == lane % 128 // 32 * 32 + lane // 128 * 16 + lane % 32 // 2).astype(f32)
    for n in range(4):
        twice.append(jnp.dot(grid[:, 128 * n : 128 * n + 128], pair, preferred_element_type=f32))
    line, lane = iota((8, 512), 0), iota((8, 512), 1)
    extra = jnp.where(line == 3, 1, jnp.where(line == 4, -4 * (lane % 2), 0)).astype(f32)
    for h in range(2):
        doubled[h] = jnp.concatenate([t[:, 128 * h : 128 * h + 128] for t in twice], axis=1) + extra
    rows16 = (iota((16, 8), 0) // 2 == iota((16, 8), 1)).astype(f32)
    columns = lax.dot_general(
        rows16, eigvec[...], (((1,), (1,)), ((), ())), precision=lax.Precision.HIGHEST, preferred_element_type=f32
    )
    for n in range(72):
        coef[n] = jnp.broadcast_to(columns[:, n : n + 1], (16, 128))

    wait(lattice.at[pl.ds(0, PEERS - 1)], lat_recv.at[0])
    def gathered(first):
        groups = []
        for n in range(PEERS // 4):
            quad = lattice[first + 4 * n : first + 4 * n + 4].astype(f32)
            groups.append(quad[0] + quad[1] + quad[2] + quad[3])
        return jnp.concatenate(groups, axis=1)

    def tabulate(vectors, which, half):
        weights = 1.0 / vectors[5:6]
        vectors = vectors.astype(bf16)
        for n in range(2):
            turns = lax.dot_general(
                doubled.at[half][:, n * 256 : (n + 1) * 256], vectors,
                (((0,), (0,)), ((), ())), preferred_element_type=f32,
            )
            turns = turns - 16.0 * jnp.floor(turns * (1.0 / 16.0))
            w = jnp.abs(turns - 8.0) - 4.0
            s = w * w
            value = w * (((float(SINE[3]) * s + float(SINE[2])) * s + float(SINE[1])) * s + float(SINE[0]))
            table.at[which, half][n * 256 : (n + 1) * 256, :] = (value * weights).astype(bf16)

    def send(unit, half):
        p = (lo + pick(STEP, core, unit)) % 4
        pltpu.make_async_remote_copy(
            y.at[unit, half], g.at[unit, hi], y_send, y_recv.at[unit],
            device_id=z_id(half, p), device_id_type=MESH,
        ).start()

    def contract(unit, half, target):
        part = jnp.dot(table[0, half], x.at[unit].reshape(1024, 128)[...], preferred_element_type=f32)
        target[...] = part.astype(bf16).reshape(PEERS, 16, 128)

    def transform(unit):
        wait(x.at[unit, pl.ds(0, PEERS - 1)], x_recv.at[unit])
        if unit in LATE:
            n = LATE.index(unit)
            for half in (0, 1):
                contract(unit, half, y.at[unit, half])
            for i, c in peers():
                pltpu.make_async_remote_copy(
                    y.at[unit, :, i * 2 + c], relayed.at[n, :, me], relay_send, relay_recv.at[n],
                    device_id=plane_id(i, c), device_id_type=MESH,
                ).start()
            relayed[n, :, me] = y[unit, :, me]
            return
        contract(unit, 1 - hi, y.at[unit, 1 - hi])
        send(unit, 1 - hi)
        if unit == 0:
            forward_lattice()
            for later in range(EARLY, JOINT):
                scatter(later)
            hand_on(lambda i: piece(held, i, hi, JOINT), 0)
            tabulate(vectors, 0, hi)
            contract(unit, hi, g.at[unit, hi])
        elif unit == 1:
            contract(unit, hi, y.at[unit, hi])

            @pl.when(core == 0)
            def keep():
                g[unit, hi] = y[unit, hi]

            pl.when(core == 1)(lambda: send(unit, hi))
        else:
            contract(unit, hi, y.at[unit, hi])
            send(unit, hi)

    vectors = gathered(0)
    tabulate(vectors, 0, 1 - hi)

    def forward_lattice():
        wait(partner, lat_recv.at[1])
        for i, c in peers():
            pltpu.make_async_remote_copy(
                partner, lattice.at[PEERS + me], lat_send, lat_recv.at[2],
                device_id=plane_id(i, c), device_id_type=MESH,
            ).start()
        lattice[PEERS + me] = partner[...]

    def forward_raw():
        wait(raw, raw_sem.at[1])
        hand_on(lambda i: raw.at[i // 8, :, i % 8], 1)

    def tabulate_others():
        wait(lattice.at[pl.ds(0, PEERS - 1)], lat_recv.at[2])

        @pl.when(core == hi)
        def active():
            vectors = gathered(PEERS)
            for half in (0, 1):
                tabulate(vectors, 1, half)

    def transform_joint():
        @pl.when(core == hi)
        def active():
            wait(x.at[pl.ds(0, 2), pl.ds(0, PEERS - 1)], joint_sem.at[1])
            for half in (0, 1):
                part = sum(
                    jnp.dot(table[n, half], joined.at[n].reshape(1024, 128)[...], preferred_element_type=f32)
                    for n in range(2)
                )
                y[JOINT, half] = part.astype(bf16).reshape(PEERS, 16, 128)
            for i, c in peers():
                pltpu.make_async_remote_copy(
                    y.at[JOINT, :, i * 2 + c], joint_relayed.at[:, chip], relay_send, relay_recv.at[2],
                    device_id=plane_id(i, c), device_id_type=MESH,
                ).start()
            joint_relayed[:, chip] = y[JOINT, :, me]

    def relay_joint():
        pl.when(core == hi)(lambda: wait(x.at[0, pl.ds(0, 15)], relay_recv.at[2]))
        pl.when(core != hi)(lambda: wait(x.at[0, pl.ds(0, 16)], relay_recv.at[2]))
        for half in (0, 1):
            pltpu.make_async_remote_copy(
                joint_relayed.at[half], joint_g.at[hi], y_send, y_recv.at[JOINT],
                device_id=z_id(half, joint_p), device_id_type=MESH,
            ).start()

    def relay(unit):
        n = LATE.index(unit)
        wait(x.at[0, pl.ds(0, PEERS - 1)], relay_recv.at[n])
        for half in (0, 1):
            pltpu.make_async_remote_copy(
                relayed.at[n, half], g.at[unit, hi], y_send, y_recv.at[unit],
                device_id=z_id(half, (lo + STEP[0][unit]) % 4), device_id_type=MESH,
            ).start()

    def spread(unit):
        if unit == 0:
            wait(g.at[unit, 0], y_recv.at[unit])
        elif unit == 1:
            pl.when(core == 0)(lambda: wait(g.at[unit, 0], y_recv.at[unit]))
            pl.when(core == 1)(lambda: wait(g.at[unit], y_recv.at[unit]))
        else:
            wait(g.at[unit], y_recv.at[unit])
        total = g[unit, 0].astype(f32) + g[unit, 1].astype(f32)
        f[unit * PEERS : (unit + 1) * PEERS] = total.astype(bf16)
        step = pick(STEP, core, unit)
        mode = (chip // 8) * 3 + pick(WHICH, core, unit)
        place_of = summed.at[step, mode, chip % 8]
        for i, c in peers():
            pltpu.make_async_remote_copy(
                f.at[unit * PEERS + i * 2 + c], place_of, f_send, f_recv.at[step],
                device_id=plane_id(i, c), device_id_type=MESH,
            ).start()
        place_of[...] = f[unit * PEERS + me]

    odd = iota((16, 128), 0) % 2 == 1

    def arrived(step, late):
        made = [STEP[c][: LATE[0]].count(step) for c in (0, 1)]
        if not late:
            for c in (0, 1):
                pl.when(core == c)(lambda: wait(f.at[pl.ds(0, 16 * sum(made) - made[c])], f_recv.at[step]))
            return
        for unit in LATE:
            if step == STEP[0][unit]:
                wait(joint_g if unit == JOINT else g.at[unit], y_recv.at[unit])

    def rotate(step, modes=range(6), first=True, last=True):
        re = (lo + 4 - step) % 4

        def block(b, _):
            def value(k):
                for unit in LATE:
                    for c in (0, 1):
                        if STEP[c][unit] == step and WHICH[c][unit] == k % 3:
                            if unit == JOINT:
                                return joint_g[c, k // 3 * 8 + b].astype(f32)
                            n = (k // 3 * 8 + b) * 2 + c
                            return g[unit, 0, n].astype(f32) + g[unit, 1, n].astype(f32)
                return summed[step, k, b].astype(f32)

            plain = {k: value(k) for k in modes}
            turned = {k: jnp.where(odd, pltpu.roll(v, 1, 0), -pltpu.roll(v, 15, 0)) for k, v in plain.items()}
            for n in range(6):
                total = None if first else so_far[b, n]
                for k in modes:
                    at = (k * 6 + n) * 2
                    term = coef[at] * plain[k] + coef[at + 1] * turned[k]
                    total = term if total is None else total + term
                if last:
                    out[:, re, n, b] = total.reshape(8, 2, 128)
                else:
                    so_far[b, n] = total
            return 0

        lax.fori_loop(0, 8, block, 0, unroll=2)

    transform(0)
    transform(1)
    forward_raw()
    transform(2)
    transform(3)
    transform(4)
    tabulate_others()
    transform_joint()
    spread(0)
    relay(3)
    spread(1)
    relay(4)
    relay_joint()
    spread(2)
    wait(lattice.at[pl.ds(0, 2 * PEERS - 1)], lat_send)
    wait(raw, raw_sem.at[0])
    wait(x.at[:, pl.ds(0, PEERS - 1)], x_send)
    pl.when(core == hi)(lambda: wait(x.at[pl.ds(0, 2), pl.ds(0, 15)], joint_sem.at[0]))
    pl.when(core != hi)(lambda: wait(x.at[pl.ds(0, 2), pl.ds(0, 16)], joint_sem.at[0]))
    pl.when(core == hi)(lambda: wait(x.at[pl.ds(0, 3), pl.ds(0, PEERS - 1)], relay_send))
    pl.when(core != hi)(lambda: wait(x.at[pl.ds(0, 2), pl.ds(0, PEERS - 1)], relay_send))
    arrived(0, False)
    rotate(0)
    arrived(2, False)
    rotate(2, (0, 3), last=False)
    wait(f.at[pl.ds(0, LATE[0] * (PEERS - 1))], f_send)
    for step in (3, 1):
        arrived(step, False)
        arrived(step, True)
        rotate(step)
    arrived(2, True)
    rotate(2, (1, 2, 4, 5), first=False)
    halves = g.reshape(2 * UNITS, PEERS, 16, 128)
    pl.when(core == 0)(lambda: wait(halves.at[pl.ds(0, 9)], y_send))
    pl.when(core == 1)(lambda: wait(halves.at[pl.ds(0, 10)], y_send))


def per_device(coupling, rp_coords, degeneracy, qpoints, eigvec):
    blocks = coupling.reshape(16, 2, 6, 32, 128).transpose(0, 2, 3, 1, 4)
    vectors = eigvec.transpose(2, 3, 1, 0).reshape(72, 8)
    vmem = pl.BlockSpec(memory_space=pltpu.VMEM)
    dma = pltpu.SemaphoreType.DMA
    bf = jnp.bfloat16
    mixed = pl.pallas_call(
        exchange,
        out_shape=jax.ShapeDtypeStruct((8, 4, 6, 8, 2, 128), jnp.float32),
        in_specs=[pl.BlockSpec(memory_space=pl.ANY)] * 5,
        out_specs=vmem,
        scratch_shapes=[
            pltpu.VMEM((3, 16), jnp.int32),
            pltpu.VMEM((1, 16), jnp.int32),
            pltpu.VMEM((3, 512), jnp.int32),
            pltpu.VMEM((72, 8), jnp.float32),
            pltpu.VMEM((16, 6, 32, 2, 128), bf),
            pltpu.VMEM((JOINT, PEERS, 16, 2, 128), bf),
            pltpu.VMEM((8, 128), bf),
            pltpu.VMEM((2 * PEERS, 8, 128), bf),
            pltpu.VMEM((2, 2, 512, 1024), bf),
            pltpu.VMEM((UNITS, 2, PEERS, 16, 128), bf),
            pltpu.VMEM((UNITS, 2, PEERS, 16, 128), bf),
            pltpu.VMEM((UNITS * PEERS, 16, 128), bf),
            pltpu.VMEM((4, 6, 8, 16, 128), bf),
            pltpu.VMEM((72, 16, 128), jnp.float32),
            pltpu.VMEM((2, 8, 512), jnp.float32),
            pltpu.VMEM((2, 2, PEERS, 16, 128), bf),
            pltpu.VMEM((2, PEERS, 16, 2, 128), bf),
            pltpu.VMEM((8, 128), bf),
            pltpu.VMEM((2, 16, 8, 2, 128), bf),
            pltpu.VMEM((2, 16, 16, 128), bf),
            pltpu.VMEM((2, 16, 16, 128), bf),
            pltpu.VMEM((8, 6, 16, 128), jnp.float32),
            dma, dma((4,)), dma, dma((3,)), dma((2,)), dma((2,)), dma, dma((3,)),
            dma, dma((JOINT,)), dma, dma((UNITS,)), dma, dma((4,)),
        ],
        compiler_params=pltpu.CompilerParams(
            collective_id=0, has_side_effects=True, vmem_limit_bytes=40 * 2**20
        ),
        name="exchange",
    )(*(pltpu.with_memory_space_constraint(v, pltpu.HBM) for v in (rp_coords, degeneracy.reshape(1, 16), qpoints, vectors, blocks)))
    return mixed.transpose(0, 1, 4, 2, 3, 5).reshape(8, 4, 2, 6, 1024)


def solution(mesh):
    return jax.shard_map(
        per_device,
        mesh=mesh,
        in_specs=(
            P("rp", "re", None, None, None),
            P(None, "rp"),
            P("rp"),
            P(),
            P("rp", None, None, None),
        ),
        out_specs=P("rp", None, None, None, "re"),
        check_vma=False,
    )
```

```python
import functools
import math

import numpy as np

import jax
import jax.numpy as jnp
from jax import lax
from jax.experimental import pallas as pl
from jax.experimental.pallas import tpu as pltpu
from jax.sharding import PartitionSpec as P

MESH = pl.DeviceIdType.MESH
UNITS = 6
PEERS = 32
LATE = (3, 4, 5)
JOINT = 5
EARLY = 3
STEP = ((0, 0, 2, 3, 1, 2), (0, 3, 1, 3, 1, 2))
WHICH = ((0, 2, 0, 0, 0, 2), (1, 2, 2, 1, 1, 1))
PLANE = ((2, 2), (2, 1), (1, 2), (2, 3), (3, 2), (1, 1), (3, 3), (1, 3), (3, 1), (2, 0), (0, 2), (0, 1), (1, 0), (0, 3), (3, 0))
SINE = np.linalg.solve(
    np.array([[w ** (2 * i + 1) for i in range(4)] for w in (1.0, 2.0, 3.0, 4.0)]),
    np.sin(np.pi / 8 * np.arange(1, 5)),
)


def place():
    rp, lo = lax.axis_index("rp"), lax.axis_index("re")
    return rp // 16, (rp // 4) % 4, (rp // 2) % 2, rp % 2, lo


def pick(table, core, unit):
    if isinstance(core, int):
        return table[core][unit]
    return jnp.where(core == 0, table[0][unit], table[1][unit])


def exchange(coords_in, degeneracy_in, points_in, eigvec_in, coupling, out, coords, degeneracy, points, eigvec, held, x, own, lattice, table, y, g, f, summed, coef, doubled, relayed, joined, partner, raw, joint_relayed, joint_g, so_far,
             load_sem, small_sem, lat_send, lat_recv, raw_sem, joint_sem, relay_send, relay_recv,
             x_send, x_recv, y_send, y_recv, f_send, f_recv):
    row, col, hi, core, lo = place()
    chip = row * 4 + col
    me = chip * 2 + core
    f32, bf16 = jnp.float32, jnp.bfloat16

    def plane_peer(d):
        r, c = (row + d[0]) % 4, (col + d[1]) % 4
        return r * 4 + c

    def peers():
        for c in (0, 1):
            for d in PLANE:
                yield plane_peer(d), c
        yield chip, 1 - core

    def plane_id(i, c):
        return ((i * 2 + hi) * 2 + c, lo)

    def z_id(z_hi, z_lo):
        return ((chip * 2 + z_hi) * 2 + core, z_lo)

    def iota(shape, dim):
        return lax.broadcasted_iota(jnp.int32, shape, dim)

    load = pltpu.make_async_copy(coupling, held, load_sem)
    small = [
        pltpu.make_async_copy(src, dst, small_sem.at[n])
        for n, (src, dst) in enumerate(
            ((coords_in, coords), (degeneracy_in, degeneracy), (points_in, points), (eigvec_in, eigvec))
        )
    ]
    for copy in small:
        copy.start()
    load.start()
    barrier = pltpu.get_barrier_semaphore()
    for i, c in peers():
        pl.semaphore_signal(barrier, inc=1, device_id=plane_id(i, c), device_id_type=MESH)
    for d in range(1, 8):
        z = (hi * 4 + lo + d) % 8
        pl.semaphore_signal(barrier, inc=1, device_id=z_id(z // 4, z % 4), device_id_type=MESH)

    pl.semaphore_wait(barrier, PEERS - 1 + 7)
    for copy in small:
        copy.wait()
    zeros = functools.partial(jnp.zeros, dtype=f32)
    stacked = jnp.concatenate(
        [coords[...].astype(f32), zeros((2, 16)), degeneracy[...].astype(f32), zeros((2, 16))], axis=0
    )
    spread16 = (iota((16, 128), 0) == iota((16, 128), 1) % 32 // 2).astype(f32)
    lat = jnp.dot(stacked, spread16, preferred_element_type=f32)
    line, lane = iota((8, 128), 0), iota((8, 128), 1)
    lat = lat + jnp.where(line == 3, 4 * (lane % 2), jnp.where(line == 4, 1, 0)).astype(f32)
    own[...] = jnp.where(lane // 32 == me % 4, lat, 0.0).astype(bf16)
    lattice[me] = own[...]

    pltpu.make_async_remote_copy(
        own, partner, lat_send, lat_recv.at[1], device_id=z_id(1 - hi, lo), device_id_type=MESH
    ).start()
    load.wait()
    joint_p = (lo + STEP[0][JOINT]) % 4
    for n in range(2):
        pltpu.make_async_remote_copy(
            held.at[:, 3 * n + pick(WHICH, 1 - hi, JOINT), pl.ds(joint_p * 8, 8)], raw.at[n],
            raw_sem.at[0], raw_sem.at[1], device_id=z_id(1 - hi, lo), device_id_type=MESH,
        ).start()

    for i, c in peers():
        pltpu.make_async_remote_copy(
            own, lattice.at[me], lat_send, lat_recv.at[0],
            device_id=plane_id(i, c), device_id_type=MESH,
        ).start()
    def piece(ref, i, c, unit):
        p = (lo + pick(STEP, c, unit)) % 4
        mode = (i // 8) * 3 + pick(WHICH, c, unit)
        return ref.at[:, mode, p * 8 + i % 8]

    def scatter(unit):
        for i, c in peers():
            pltpu.make_async_remote_copy(
                piece(held, i, c, unit), x.at[unit, me], x_send, x_recv.at[unit],
                device_id=plane_id(i, c), device_id_type=MESH,
            ).start()

    for unit in range(EARLY):
        scatter(unit)

    def hand_on(source, n):
        def to(i):
            pltpu.make_async_remote_copy(
                source(i), joined.at[n, me], joint_sem.at[0], joint_sem.at[1],
                device_id=plane_id(i, hi), device_id_type=MESH,
            ).start()

        for d in PLANE:
            to(plane_peer(d))
        pl.when(core != hi)(lambda: to(chip))

        @pl.when(core == hi)
        def keep():
            joined[n, me] = source(chip)[...]

    for unit in range(JOINT):
        x[unit, me] = piece(held, chip, core, unit)[...]

    def wait(ref, sem):
        pltpu.make_async_copy(ref, ref, sem).wait()

    grid = jnp.concatenate([points[...].astype(f32), zeros((5, 512))], axis=0)
    twice = []
    lane = iota((128, 256), 1)
    pair = (iota((128, 256), 0) == lane % 128 // 32 * 32 + lane // 128 * 16 + lane % 32 // 2).astype(f32)
    for n in range(4):
        twice.append(jnp.dot(grid[:, 128 * n : 128 * n + 128], pair, preferred_element_type=f32))
    line, lane = iota((8, 512), 0), iota((8, 512), 1)
    extra = jnp.where(line == 3, 1, jnp.where(line == 4, -4 * (lane % 2), 0)).astype(f32)
    for h in range(2):
        doubled[h] = jnp.concatenate([t[:, 128 * h : 128 * h + 128] for t in twice], axis=1) + extra
    rows16 = (iota((16, 8), 0) // 2 == iota((16, 8), 1)).astype(f32)
    columns = lax.dot_general(
        rows16, eigvec[...], (((1,), (1,)), ((), ())), precision=lax.Precision.HIGHEST, preferred_element_type=f32
    )
    for n in range(72):
        coef[n] = jnp.broadcast_to(columns[:, n : n + 1], (16, 128))

    wait(lattice.at[pl.ds(0, PEERS - 1)], lat_recv.at[0])
    def gathered(first):
        groups = []
        for n in range(PEERS // 4):
            quad = lattice[first + 4 * n : first + 4 * n + 4].astype(f32)
            groups.append(quad[0] + quad[1] + quad[2] + quad[3])
        return jnp.concatenate(groups, axis=1)

    def tabulate(vectors, which, half):
        weights = 1.0 / vectors[5:6]
        vectors = vectors.astype(bf16)
        for n in range(2):
            turns = lax.dot_general(
                doubled.at[half][:, n * 256 : (n + 1) * 256], vectors,
                (((0,), (0,)), ((), ())), preferred_element_type=f32,
            )
            turns = turns - 16.0 * jnp.floor(turns * (1.0 / 16.0))
            w = jnp.abs(turns - 8.0) - 4.0
            s = w * w
            value = w * (((float(SINE[3]) * s + float(SINE[2])) * s + float(SINE[1])) * s + float(SINE[0]))
            table.at[which, half][n * 256 : (n + 1) * 256, :] = (value * weights).astype(bf16)

    def send(unit, half):
        p = (lo + pick(STEP, core, unit)) % 4
        pltpu.make_async_remote_copy(
            y.at[unit, half], g.at[unit, hi], y_send, y_recv.at[unit],
            device_id=z_id(half, p), device_id_type=MESH,
        ).start()

    def contract(unit, half, target):
        part = jnp.dot(table[0, half], x.at[unit].reshape(1024, 128)[...], preferred_element_type=f32)
        target[...] = part.astype(bf16).reshape(PEERS, 16, 128)

    def transform(unit):
        wait(x.at[unit, pl.ds(0, PEERS - 1)], x_recv.at[unit])
        if unit in LATE:
            n = LATE.index(unit)
            for half in (0, 1):
                contract(unit, half, y.at[unit, half])
            for i, c in peers():
                pltpu.make_async_remote_copy(
                    y.at[unit, :, i * 2 + c], relayed.at[n, :, me], relay_send, relay_recv.at[n],
                    device_id=plane_id(i, c), device_id_type=MESH,
                ).start()
            relayed[n, :, me] = y[unit, :, me]
            return
        contract(unit, 1 - hi, y.at[unit, 1 - hi])
        send(unit, 1 - hi)
        if unit == 0:
            forward_lattice()
            for later in range(EARLY, JOINT):
                scatter(later)
            hand_on(lambda i: piece(held, i, hi, JOINT), 0)
            tabulate(vectors, 0, hi)
            contract(unit, hi, g.at[unit, hi])
        elif unit == 1:
            contract(unit, hi, y.at[unit, hi])

            @pl.when(core == 0)
            def keep():
                g[unit, hi] = y[unit, hi]

            pl.when(core == 1)(lambda: send(unit, hi))
        else:
            contract(unit, hi, y.at[unit, hi])
            send(unit, hi)

    vectors = gathered(0)
    tabulate(vectors, 0, 1 - hi)

    def forward_lattice():
        wait(partner, lat_recv.at[1])
        for i, c in peers():
            pltpu.make_async_remote_copy(
                partner, lattice.at[PEERS + me], lat_send, lat_recv.at[2],
                device_id=plane_id(i, c), device_id_type=MESH,
            ).start()
        lattice[PEERS + me] = partner[...]

    def forward_raw():
        wait(raw, raw_sem.at[1])
        hand_on(lambda i: raw.at[i // 8, :, i % 8], 1)

    def tabulate_others():
        wait(lattice.at[pl.ds(0, PEERS - 1)], lat_recv.at[2])

        @pl.when(core == hi)
        def active():
            vectors = gathered(PEERS)
            for half in (0, 1):
                tabulate(vectors, 1, half)

    def transform_joint():
        @pl.when(core == hi)
        def active():
            wait(x.at[pl.ds(0, 2), pl.ds(0, PEERS - 1)], joint_sem.at[1])
            for half in (0, 1):
                part = sum(
                    jnp.dot(table[n, half], joined.at[n].reshape(1024, 128)[...], preferred_element_type=f32)
                    for n in range(2)
                )
                y[JOINT, half] = part.astype(bf16).reshape(PEERS, 16, 128)
            for i, c in peers():
                pltpu.make_async_remote_copy(
                    y.at[JOINT, :, i * 2 + c], joint_relayed.at[:, chip], relay_send, relay_recv.at[2],
                    device_id=plane_id(i, c), device_id_type=MESH,
                ).start()
            joint_relayed[:, chip] = y[JOINT, :, me]

    def relay_joint():
        pl.when(core == hi)(lambda: wait(x.at[0, pl.ds(0, 15)], relay_recv.at[2]))
        pl.when(core != hi)(lambda: wait(x.at[0, pl.ds(0, 16)], relay_recv.at[2]))
        for half in (0, 1):
            pltpu.make_async_remote_copy(
                joint_relayed.at[half], joint_g.at[hi], y_send, y_recv.at[JOINT],
                device_id=z_id(half, joint_p), device_id_type=MESH,
            ).start()

    def relay(unit):
        n = LATE.index(unit)
        wait(x.at[0, pl.ds(0, PEERS - 1)], relay_recv.at[n])
        for half in (0, 1):
            pltpu.make_async_remote_copy(
                relayed.at[n, half], g.at[unit, hi], y_send, y_recv.at[unit],
                device_id=z_id(half, (lo + STEP[0][unit]) % 4), device_id_type=MESH,
            ).start()

    def spread(unit):
        if unit == 0:
            wait(g.at[unit, 0], y_recv.at[unit])
        elif unit == 1:
            pl.when(core == 0)(lambda: wait(g.at[unit, 0], y_recv.at[unit]))
            pl.when(core == 1)(lambda: wait(g.at[unit], y_recv.at[unit]))
        else:
            wait(g.at[unit], y_recv.at[unit])
        total = g[unit, 0].astype(f32) + g[unit, 1].astype(f32)
        f[unit * PEERS : (unit + 1) * PEERS] = total.astype(bf16)
        step = pick(STEP, core, unit)
        mode = (chip // 8) * 3 + pick(WHICH, core, unit)
        place_of = summed.at[step, mode, chip % 8]
        for i, c in peers():
            pltpu.make_async_remote_copy(
                f.at[unit * PEERS + i * 2 + c], place_of, f_send, f_recv.at[step],
                device_id=plane_id(i, c), device_id_type=MESH,
            ).start()
        place_of[...] = f[unit * PEERS + me]

    odd = iota((16, 128), 0) % 2 == 1

    def arrived(step, late):
        made = [STEP[c][: LATE[0]].count(step) for c in (0, 1)]
        if not late:
            for c in (0, 1):
                pl.when(core == c)(lambda: wait(f.at[pl.ds(0, 16 * sum(made) - made[c])], f_recv.at[step]))
            return
        for unit in LATE:
            if step == STEP[0][unit]:
                wait(joint_g if unit == JOINT else g.at[unit], y_recv.at[unit])

    def rotate(step, modes=range(6), first=True, last=True):
        re = (lo + 4 - step) % 4

        def block(b, _):
            def value(k):
                for unit in LATE:
                    for c in (0, 1):
                        if STEP[c][unit] == step and WHICH[c][unit] == k % 3:
                            if unit == JOINT:
                                return joint_g[c, k // 3 * 8 + b].astype(f32)
                            n = (k // 3 * 8 + b) * 2 + c
                            return g[unit, 0, n].astype(f32) + g[unit, 1, n].astype(f32)
                return summed[step, k, b].astype(f32)

            plain = {k: value(k) for k in modes}
            turned = {k: jnp.where(odd, pltpu.roll(v, 1, 0), -pltpu.roll(v, 15, 0)) for k, v in plain.items()}
            for n in range(6):
                total = None if first else so_far[b, n]
                for k in modes:
                    at = (k * 6 + n) * 2
                    term = coef[at] * plain[k] + coef[at + 1] * turned[k]
                    total = term if total is None else total + term
                if last:
                    out[:, re, n, b] = total.reshape(8, 2, 128)
                else:
                    so_far[b, n] = total
            return 0

        lax.fori_loop(0, 8, block, 0, unroll=4)

    transform(0)
    transform(1)
    forward_raw()
    transform(2)
    transform(3)
    transform(4)
    tabulate_others()
    transform_joint()
    spread(0)
    relay(3)
    spread(1)
    relay(4)
    relay_joint()
    spread(2)
    wait(lattice.at[pl.ds(0, 2 * PEERS - 1)], lat_send)
    wait(raw, raw_sem.at[0])
    wait(x.at[:, pl.ds(0, PEERS - 1)], x_send)
    pl.when(core == hi)(lambda: wait(x.at[pl.ds(0, 2), pl.ds(0, 15)], joint_sem.at[0]))
    pl.when(core != hi)(lambda: wait(x.at[pl.ds(0, 2), pl.ds(0, 16)], joint_sem.at[0]))
    pl.when(core == hi)(lambda: wait(x.at[pl.ds(0, 3), pl.ds(0, PEERS - 1)], relay_send))
    pl.when(core != hi)(lambda: wait(x.at[pl.ds(0, 2), pl.ds(0, PEERS - 1)], relay_send))
    arrived(0, False)
    rotate(0)
    arrived(2, False)
    rotate(2, (0, 3), last=False)
    wait(f.at[pl.ds(0, LATE[0] * (PEERS - 1))], f_send)
    for step in (3, 1):
        arrived(step, False)
        arrived(step, True)
        rotate(step)
    arrived(2, True)
    rotate(2, (1, 2, 4, 5), first=False)
    halves = g.reshape(2 * UNITS, PEERS, 16, 128)
    pl.when(core == 0)(lambda: wait(halves.at[pl.ds(0, 9)], y_send))
    pl.when(core == 1)(lambda: wait(halves.at[pl.ds(0, 10)], y_send))


def per_device(coupling, rp_coords, degeneracy, qpoints, eigvec):
    blocks = coupling.reshape(16, 2, 6, 32, 128).transpose(0, 2, 3, 1, 4)
    vectors = eigvec.transpose(2, 3, 1, 0).reshape(72, 8)
    vmem = pl.BlockSpec(memory_space=pltpu.VMEM)
    dma = pltpu.SemaphoreType.DMA
    bf = jnp.bfloat16
    mixed = pl.pallas_call(
        exchange,
        out_shape=jax.ShapeDtypeStruct((8, 4, 6, 8, 2, 128), jnp.float32),
        in_specs=[pl.BlockSpec(memory_space=pl.ANY)] * 5,
        out_specs=vmem,
        scratch_shapes=[
            pltpu.VMEM((3, 16), jnp.int32),
            pltpu.VMEM((1, 16), jnp.int32),
            pltpu.VMEM((3, 512), jnp.int32),
            pltpu.VMEM((72, 8), jnp.float32),
            pltpu.VMEM((16, 6, 32, 2, 128), bf),
            pltpu.VMEM((JOINT, PEERS, 16, 2, 128), bf),
            pltpu.VMEM((8, 128), bf),
            pltpu.VMEM((2 * PEERS, 8, 128), bf),
            pltpu.VMEM((2, 2, 512, 1024), bf),
            pltpu.VMEM((UNITS, 2, PEERS, 16, 128), bf),
            pltpu.VMEM((UNITS, 2, PEERS, 16, 128), bf),
            pltpu.VMEM((UNITS * PEERS, 16, 128), bf),
            pltpu.VMEM((4, 6, 8, 16, 128), bf),
            pltpu.VMEM((72, 16, 128), jnp.float32),
            pltpu.VMEM((2, 8, 512), jnp.float32),
            pltpu.VMEM((2, 2, PEERS, 16, 128), bf),
            pltpu.VMEM((2, PEERS, 16, 2, 128), bf),
            pltpu.VMEM((8, 128), bf),
            pltpu.VMEM((2, 16, 8, 2, 128), bf),
            pltpu.VMEM((2, 16, 16, 128), bf),
            pltpu.VMEM((2, 16, 16, 128), bf),
            pltpu.VMEM((8, 6, 16, 128), jnp.float32),
            dma, dma((4,)), dma, dma((3,)), dma((2,)), dma((2,)), dma, dma((3,)),
            dma, dma((JOINT,)), dma, dma((UNITS,)), dma, dma((4,)),
        ],
        compiler_params=pltpu.CompilerParams(
            collective_id=0, has_side_effects=True, vmem_limit_bytes=40 * 2**20
        ),
        name="exchange",
    )(*(pltpu.with_memory_space_constraint(v, pltpu.HBM) for v in (rp_coords, degeneracy.reshape(1, 16), qpoints, vectors, blocks)))
    return mixed.transpose(0, 1, 4, 2, 3, 5).reshape(8, 4, 2, 6, 1024)


def solution(mesh):
    return jax.shard_map(
        per_device,
        mesh=mesh,
        in_specs=(
            P("rp", "re", None, None, None),
            P(None, "rp"),
            P("rp"),
            P(),
            P("rp", None, None, None),
        ),
        out_specs=P("rp", None, None, None, "re"),
        check_vma=False,
    )
```
